512 devices in a mesh: tm: 8 (over z), height: 8 (over y_hi, core), heads: 8 (over x, y_lo).
Axes of the slice: x: 4, y: 8 (y_hi: 4, y_lo: 2; y = y_hi * 2 + y_lo), z: 8, core: 2. Of those that a mesh axis runs over, the one named last changes fastest.
Arguments:
- grad_output: bfloat16 [8, 8, 384, 3072], P('tm', 'height', None, 'heads'), may hold values from -6 to 6
- out_weight: bfloat16 [2048, 3072], P(None, 'heads'), may hold values from -0.109375 to 0.109375
- queries: bfloat16 [8, 8, 384, 2048], P('tm', 'height', None, 'heads'), may hold values from -24 to 24
- key_states: bfloat16 [8, 8, 384, 2048], P('tm', 'height', None, 'heads'), may hold values from -4 to 4
- value_states: bfloat16 [8, 8, 384, 2048], P('tm', 'height', None, 'heads'), may hold values from -6 to 6
- window: int32 [8, 8, 1, 27], replicated, may hold values from 0 to 1, as said below
Outputs:
- query_grad: bfloat16 [8, 8, 384, 2048], P('tm', 'height', None, 'heads')
- key_grad: bfloat16 [8, 8, 384, 2048], P('tm', 'height', None, 'heads')
- value_grad: bfloat16 [8, 8, 384, 2048], P('tm', 'height', None, 'heads')
The draws below stay inside these ranges and needn't reach their ends.
Inputs may be any that keep to these rules, and one draw needn't show every extreme that they name: window[t, h, w, 9(a+1) + 3(b+1) + (c+1)] is 1 where query tile (t, h, w) attends key tile (t+a, h+b, w+c), a, b, c each -1, 0 or 1; it is 1 at index 13 (the tile itself) and 0 where the key tile lies outside the video.
All inputs are finite; a program needn't handle non-finite values.
Results may differ from the reference program's by a relative error of at most 0.02.
Values may be sent and summed in bfloat16 or wider, within the bound.
A program may use at most 64 MiB of HBM per device.

```python
import jax
import jax.numpy as jnp
from jax import lax

D = 3072
HEADS = 16
HD = 128
TILE = 384
TW = 1
TT = 8
TH = 8
DCHUNK = 384
N_HEADS = 8


def draw_both(key):
    tokens = TW * TILE
    shape = (TT, TH, tokens, HEADS * HD)
    base_key = jax.random.fold_in(key, 71)
    first_key, second_key = jax.random.split(base_key)
    keys_drawn = jnp.clip(jax.random.normal(first_key, shape, jnp.float32), -4.0, 4.0)
    queries_drawn = jnp.clip(jax.random.normal(second_key, shape, jnp.float32), -4.0, 4.0)
    return (queries_drawn, keys_drawn)


def draw_queries(key, part):
    queries_drawn, keys_drawn = draw_both(key)
    return queries_drawn.astype(jnp.bfloat16)


def draw_key_states(key, part):
    queries_drawn, keys_drawn = draw_both(key)
    return keys_drawn.astype(jnp.bfloat16)


def draw_window(key, part):
    base_key = jax.random.fold_in(key, 13)
    level_key, roll_key = jax.random.split(base_key)
    ladder = jax.random.randint(level_key, (TT, TH, 1, 1), 0, 4)
    levels = ladder * ladder
    rolled = jax.random.randint(roll_key, (TT, TH, TW, 27), 0, 16)
    offset = jnp.arange(27)
    time_pos = jnp.arange(TT)[:, None, None, None] + (offset // 9 - 1)[None, None, None, :]
    height_pos = jnp.arange(TH)[None, :, None, None] + (offset // 3 % 3 - 1)[None, None, None, :]
    width_pos = jnp.arange(TW)[None, None, :, None] + (offset % 3 - 1)[None, None, None, :]
    inside = (time_pos >= 0) & (time_pos < TT) & (height_pos >= 0) & (height_pos < TH) & (width_pos >= 0) & (width_pos < TW)
    active = ((rolled < levels) | (offset == 13)[None, None, None, :]) & inside
    return active.astype(jnp.int32)


def level_of(rng, extent, cuts, low, high):
    factor_of, own = 1.0, jax.random.fold_in(rng, 6)
    for dim, blocks in cuts:
        heights = jnp.exp(jax.random.uniform(jax.random.fold_in(own, dim), (blocks,), jnp.float32, low / len(cuts), high / len(cuts)))
        factor_of = factor_of * jnp.repeat(heights, extent[dim] // blocks).reshape([-1 if axis == dim else 1 for axis in range(len(extent))])
    return factor_of


def gaussian(rng, extent, deviation, bound, pieces=(), kind=jnp.bfloat16):
    values = jax.random.normal(rng, extent, jnp.float32) * deviation
    if len(pieces) > 0:
        values = level_of(rng, extent, pieces, -0.22, 0.18) * values
    return jnp.clip(values, min=-bound, max=bound).astype(kind)


def setup_inputs(seed: int = 0) -> dict:
    keys = jax.random.split(jax.random.key(seed), 7)
    grad_output = gaussian(keys[0], (TT, TH, TW * TILE, D), 1.0, 6.0, ((0, 8), (1, 8), (3, 8)))
    out_weight = gaussian(keys[1], (HEADS * HD, D), D ** -0.5, 0.109375, ((1, 8),))
    queries = draw_queries(jax.random.fold_in(keys[6], 71), 0)
    key_states = draw_key_states(jax.random.fold_in(keys[6], 71), 0)
    value_states = gaussian(keys[4], (TT, TH, TW * TILE, HEADS * HD), 1.0, 6.0, ((0, 8), (1, 8), (3, 8)))
    window = draw_window(jax.random.fold_in(keys[6], 71), 0)
    return dict(grad_output=grad_output, out_weight=out_weight, queries=queries, key_states=key_states, value_states=value_states, window=window)


lowest = -1.0e30


def rounded(values):
    return lax.optimization_barrier(values.astype(jnp.bfloat16)).astype(jnp.float32)


def neighbour(tile_index, offset, sign):
    time_pos = tile_index // (TH * TW) + sign * (offset // 9 - 1)
    height_pos = (tile_index // TW) % TH + sign * ((offset // 3) % 3 - 1)
    width_pos = tile_index % TW + sign * (offset % 3 - 1)
    inside = (time_pos >= 0) & (time_pos < TT) & (height_pos >= 0) & (height_pos < TH) & (width_pos >= 0) & (width_pos < TW)
    clipped = jnp.clip(time_pos, 0, TT - 1) * (TH * TW) + jnp.clip(height_pos, 0, TH - 1) * TW + jnp.clip(width_pos, 0, TW - 1)
    return inside, clipped.astype(jnp.int32)


def reference(grad_output, out_weight, queries, key_states, value_states, window):
    scaling = HD ** -0.5
    grad_rows = grad_output.reshape(-1, D)
    summed = jnp.zeros((grad_rows.shape[0], HEADS * HD), jnp.float32)
    for part in range(N_HEADS):
        term = lax.dot_general(grad_rows[:, part * DCHUNK:(part + 1) * DCHUNK], out_weight[:, part * DCHUNK:(part + 1) * DCHUNK], (((1,), (1,)), ((), ())), preferred_element_type=jnp.float32)
        summed = summed + rounded(term)
    tile_total = TT * TH * TW
    grad_tiles = summed.astype(jnp.bfloat16).reshape(tile_total, TILE, HEADS, HD)
    query_tiles = queries.reshape(tile_total, TILE, HEADS, HD)
    key_tiles = key_states.reshape(tile_total, TILE, HEADS, HD)
    value_tiles = value_states.reshape(tile_total, TILE, HEADS, HD)
    windows = window.reshape(tile_total, 27)
    indices = jnp.arange(tile_total, dtype=jnp.int32)
    offsets = jnp.arange(27, dtype=jnp.int32)

    def scores_of(query_index, key_index):
        query_tile = query_tiles[query_index].astype(jnp.float32)
        grad_tile = grad_tiles[query_index].astype(jnp.float32)
        key_tile = key_tiles[key_index].astype(jnp.float32)
        value_tile = value_tiles[key_index].astype(jnp.float32)
        scores = jnp.einsum("qhd,khd->hqk", query_tile, key_tile) * scaling
        slopes = jnp.einsum("qhd,khd->hqk", grad_tile, value_tile)
        return scores, slopes

    def tile_stats(query_index):
        def visit(carried, offset):
            inside, key_index = neighbour(query_index, offset, 1)
            active = inside & (windows[query_index, offset] == 1)

            def include(current):
                highest, totals, weighted = current
                scores, slopes = scores_of(query_index, key_index)
                renewed = jnp.maximum(highest, jnp.max(scores, axis=2))
                factor = jnp.exp(highest - renewed)
                weights = jnp.exp(scores - renewed[:, :, None])
                return renewed, totals * factor + jnp.sum(weights, axis=2), weighted * factor + jnp.sum(weights * slopes, axis=2)

            return lax.cond(active, include, lambda unchanged: unchanged, carried), None

        start_state = (jnp.full((HEADS, TILE), lowest, jnp.float32), jnp.zeros((HEADS, TILE), jnp.float32), jnp.zeros((HEADS, TILE), jnp.float32))
        final_state, unused = lax.scan(visit, start_state, offsets)
        highest, totals, weighted = final_state
        return highest + jnp.log(totals), weighted / totals

    log_totals, mean_slopes = lax.map(tile_stats, indices)

    def tile_query(query_index):
        def visit(running, offset):
            inside, key_index = neighbour(query_index, offset, 1)
            active = inside & (windows[query_index, offset] == 1)

            def include(previous):
                scores, slopes = scores_of(query_index, key_index)
                probabilities = jnp.exp(scores - log_totals[query_index][:, :, None])
                score_grads = rounded(probabilities * (slopes - mean_slopes[query_index][:, :, None]))
                return previous + jnp.einsum("hqk,khd->qhd", score_grads, key_tiles[key_index].astype(jnp.float32))

            return lax.cond(active, include, lambda unchanged: unchanged, running), None

        summed_grads, unused = lax.scan(visit, jnp.zeros((TILE, HEADS, HD), jnp.float32), offsets)
        return (scaling * summed_grads).astype(jnp.bfloat16)

    def tile_key(key_index):
        def visit(carried, offset):
            inside, query_index = neighbour(key_index, offset, -1)
            active = inside & (windows[query_index, offset] == 1)

            def include(previous):
                key_sum, value_sum = previous
                scores, slopes = scores_of(query_index, key_index)
                probabilities = jnp.exp(scores - log_totals[query_index][:, :, None])
                score_grads = rounded(probabilities * (slopes - mean_slopes[query_index][:, :, None]))
                value_sum = value_sum + jnp.einsum("hqk,qhd->khd", rounded(probabilities), grad_tiles[query_index].astype(jnp.float32))
                key_sum = key_sum + jnp.einsum("hqk,qhd->khd", score_grads, query_tiles[query_index].astype(jnp.float32))
                return key_sum, value_sum

            return lax.cond(active, include, lambda unchanged: unchanged, carried), None

        start_sums = (jnp.zeros((TILE, HEADS, HD), jnp.float32), jnp.zeros((TILE, HEADS, HD), jnp.float32))
        final_sums, unused = lax.scan(visit, start_sums, offsets)
        return (scaling * final_sums[0]).astype(jnp.bfloat16), final_sums[1].astype(jnp.bfloat16)

    query_grad = lax.map(tile_query, indices)
    key_grad, value_grad = lax.map(tile_key, indices)
    shape = (TT, TH, TW * TILE, HEADS * HD)
    return query_grad.reshape(shape), key_grad.reshape(shape), value_grad.reshape(shape)
```

```python
import functools

import jax
import jax.numpy as jnp
from jax import lax
from jax.experimental import pallas as pl
from jax.experimental.pallas import tpu as pltpu
from jax.sharding import PartitionSpec as P

HD = 128
TILE = 384
FEAT = 256
HEADS_HERE = 2
CHUNKS = 3
ROWS = TILE // CHUNKS
RING_X = 4
LOG2E = 1.4426950408889634
SCALING = HD ** (-0.5)
MESH = pl.DeviceIdType.MESH

FRAME = (0, 0, -1, 1, -1, 1, 0, -1, 1)
COLUMN = (0, 1, 0, 0, 1, 1, 2, 2, 2)
SOURCE = {1: 0, 2: 0, 3: 0, 6: 0, 4: 2, 5: 3, 7: 6, 8: 6}

f32 = jnp.float32
bf16 = jnp.bfloat16


def dot_nt(a, b):
    return lax.dot_general(a, b, (((1,), (1,)), ((), ())), preferred_element_type=f32)


def dot_tn(a, b):
    return lax.dot_general(a, b, (((0,), (0,)), ((), ())), preferred_element_type=f32)


def dot_nn(a, b):
    return lax.dot_general(a, b, (((1,), (0,)), ((), ())), preferred_element_type=f32)


def loop(count, body):
    def step(index, carry):
        body(index)
        return carry

    lax.fori_loop(0, count, step, 0)


def kernel(
    frames,
    rows_of_tiles,
    go_hbm,
    w_hbm,
    q_hbm,
    k_hbm,
    v_hbm,
    win,
    dq_out,
    dk_out,
    dv_out,
    go,
    w,
    kb,
    vb,
    qb,
    db,
    lse,
    delta,
    sbuf,
    pq,
    pk,
    top,
    total,
    ot,
    dqt,
    dk,
    dv,
    own,
    rs_send,
    rs_recv,
    biases,
    load_sem,
    k_send,
    k_recv,
    v_send,
    v_recv,
    q_send,
    q_recv,
    d_send,
    d_recv,
    lse_send,
    lse_recv,
    delta_send,
    delta_recv,
    rs_ssem,
    rs_rsem,
):
    t = lax.axis_index("tm")
    h = lax.axis_index("height")
    g = lax.axis_index("heads")
    x = g // 2
    yl = g % 2
    odd = h % 2
    partner = {"height": h + 1 - 2 * odd}
    outer = {"height": (h + 2 * odd - 1 + rows_of_tiles) % rows_of_tiles}
    t_next = {"tm": (t + 1) % frames}
    t_prev = {"tm": (t + frames - 1) % frames}
    x_next = {"heads": ((x + 1) % RING_X) * 2 + yl}
    x_prev = {"heads": ((x + RING_X - 1) % RING_X) * 2 + yl}
    y_other = {"heads": x * 2 + 1 - yl}
    target = {1: partner, 4: partner, 5: partner, 2: t_next, 7: t_next, 3: t_prev, 8: t_prev, 6: outer}

    loads = [
        pltpu.make_async_copy(src, dst, load_sem.at[i])
        for i, (src, dst) in enumerate(
            (
                (k_hbm.at[0, 0], kb.at[0]),
                (v_hbm.at[0, 0], vb.at[0]),
                (go_hbm.at[0, 0], go),
                (w_hbm, w),
                (q_hbm.at[0, 0], qb.at[0]),
            )
        )
    ]
    for load in loads:
        load.start()

    barrier = pltpu.get_barrier_semaphore()
    peers = (partner, outer, t_next, t_prev, x_next, x_prev, y_other)
    for peer in peers:
        pl.semaphore_signal(barrier, inc=1, device_id=peer, device_id_type=MESH)

    sign = 1 - 2 * odd
    for slot in range(9):
        a = FRAME[slot]
        b = (0, sign, -sign)[COLUMN[slot]]
        seen = win[t, h, 0, 9 * (a + 1) + 3 * (b + 1) + 1]
        biases[0, slot] = (seen.astype(f32) - 1.0) * 1e30
        seen = win[
            (t + a + frames) % frames,
            (h + b + rows_of_tiles) % rows_of_tiles,
            0,
            9 * (1 - a) + 3 * (1 - b) + 1,
        ]
        biases[1, slot] = (seen.astype(f32) - 1.0) * 1e30

    pl.semaphore_wait(barrier, len(peers))

    def tile_copy(buf, slot, send, recv):
        return pltpu.make_async_remote_copy(
            src_ref=buf.at[SOURCE[slot]],
            dst_ref=buf.at[slot],
            send_sem=send.at[slot],
            recv_sem=recv.at[slot],
            device_id=target[slot],
            device_id_type=MESH,
        )

    def chunk_copy(slot, c):
        rows = pl.ds(pl.multiple_of(c * ROWS, ROWS), ROWS)
        return pltpu.make_async_remote_copy(
            src_ref=db.at[SOURCE[slot], rows],
            dst_ref=db.at[slot, rows],
            send_sem=d_send.at[slot, c],
            recv_sem=d_recv.at[slot, c],
            device_id=target[slot],
            device_id_type=MESH,
        )

    def arrived(buf, slot, recv):
        pltpu.make_async_copy(buf.at[slot], buf.at[slot], recv.at[slot]).wait()

    def chunk_arrived(slot, c):
        rows = pl.ds(pl.multiple_of(c * ROWS, ROWS), ROWS)
        piece = db.at[slot, rows]
        pltpu.make_async_copy(piece, piece, d_recv.at[slot, c]).wait()

    def rs_copy(kind, c):
        rows = pl.ds(pl.multiple_of(c * ROWS, ROWS), ROWS)
        return pltpu.make_async_remote_copy(
            src_ref=rs_send.at[kind, rows],
            dst_ref=rs_recv.at[kind, rows],
            send_sem=rs_ssem.at[kind, c],
            recv_sem=rs_rsem.at[kind, c],
            device_id=(x_next, x_prev, x_next, x_next, x_prev, x_prev, y_other)[kind],
            device_id_type=MESH,
        )

    def rs_arrived(kind, c):
        rows = pl.ds(pl.multiple_of(c * ROWS, ROWS), ROWS)
        piece = rs_recv.at[kind, rows]
        pltpu.make_async_copy(piece, piece, rs_rsem.at[kind, c]).wait()

    def chunk_rows(c):
        return pl.ds(pl.multiple_of(c * ROWS, ROWS), ROWS)

    def partial(column, half, c):
        block = (2 * ((x + column) % RING_X) + (yl if half == 0 else 1 - yl)) * FEAT
        return dot_nt(go[chunk_rows(c), :], w[pl.ds(pl.multiple_of(block, FEAT), FEAT), :])

    tiles = {
        "k": (kb, k_send, k_recv),
        "v": (vb, v_send, v_recv),
        "q": (qb, q_send, q_recv),
        "lse": (lse, lse_send, lse_recv),
        "delta": (delta, delta_send, delta_recv),
    }

    def start(name, *slots):
        buf, send, recv = tiles[name]
        for slot in slots:
            tile_copy(buf, slot, send, recv).start()

    def relay(name, came, *slots):
        buf, send, recv = tiles[name]
        arrived(buf, came, recv)
        start(name, *slots)

    loads[0].wait()
    start("k", 2, 3, 6, 1)
    loads[1].wait()
    start("v", 2, 3, 6, 1)
    loads[2].wait()
    loads[3].wait()

    def far(c):
        rs_send[0, chunk_rows(c), :] = partial(2, 0, c).astype(bf16)
        rs_copy(0, c).start()
        rs_send[1, chunk_rows(c), :] = partial(2, 1, c).astype(bf16)
        rs_copy(1, c).start()

    loop(CHUNKS, far)
    loads[4].wait()
    start("q", 6, 1)

    def near(c):
        rs_send[3, chunk_rows(c), :] = partial(1, 1, c).astype(bf16)
        rs_send[4, chunk_rows(c), :] = partial(3, 0, c).astype(bf16)
        own[0, chunk_rows(c), :] = partial(0, 0, c)
        own[1, chunk_rows(c), :] = partial(0, 1, c)

    loop(CHUNKS, near)

    def combine(c):
        rs_arrived(0, c)
        rs_send[2, chunk_rows(c), :] = (partial(1, 0, c) + rs_recv[0, chunk_rows(c), :].astype(f32)).astype(bf16)
        rs_copy(2, c).start()
        rs_arrived(1, c)
        rs_send[5, chunk_rows(c), :] = (partial(3, 1, c) + rs_recv[1, chunk_rows(c), :].astype(f32)).astype(bf16)
        rs_copy(5, c).start()
        rs_copy(3, c).start()
        rs_copy(4, c).start()

    loop(CHUNKS, combine)

    relay("k", 6, 7, 8)
    relay("k", 2, 4)
    relay("k", 3, 5)
    relay("v", 6, 7, 8)
    start("q", 2, 3)
    relay("v", 2, 4)
    relay("v", 3, 5)

    def cross(c):
        rs_arrived(3, c)
        rs_arrived(5, c)
        rs_send[6, chunk_rows(c), :] = (
            own[1, chunk_rows(c), :]
            + rs_recv[3, chunk_rows(c), :].astype(f32)
            + rs_recv[5, chunk_rows(c), :].astype(f32)
        ).astype(bf16)
        rs_copy(6, c).start()

    loop(CHUNKS, cross)

    def settle(c):
        rs_arrived(2, c)
        rs_arrived(4, c)
        summed = (
            own[0, chunk_rows(c), :]
            + rs_recv[2, chunk_rows(c), :].astype(f32)
            + rs_recv[4, chunk_rows(c), :].astype(f32)
        )
        rs_arrived(6, c)
        db[0, chunk_rows(c), :] = (summed + rs_recv[6, chunk_rows(c), :].astype(f32)).astype(bf16)
        for slot in (2, 3, 6, 1):
            chunk_copy(slot, c).start()

    loop(CHUNKS, settle)
    relay("q", 6, 7, 8)

    heads = [(n, slice(n * HD, (n + 1) * HD)) for n in range(HEADS_HERE)]

    lse[0] = jnp.zeros(lse.shape[1:], f32)
    delta[0] = jnp.zeros(delta.shape[1:], f32)

    top[...] = jnp.full(top.shape, -1e30, f32)
    total[...] = jnp.zeros(total.shape, f32)
    ot[...] = jnp.zeros(ot.shape, f32)

    def scores(j):
        bias = biases[0, j]
        for n, cols in heads:
            s = dot_nt(kb[j, :, cols], qb[0, :, cols]) * (SCALING * LOG2E) + bias
            sbuf[j, n] = s
            top[n] = jnp.maximum(top[n], jnp.max(s, axis=0, keepdims=True))

    def weights(j):
        for n, cols in heads:
            p = jnp.exp2(sbuf[j, n] - top[n])
            total[n] += jnp.sum(p, axis=0, keepdims=True)
            p = p.astype(bf16)
            pq[j, n] = p
            ot[n] += dot_tn(vb[j, :, cols], p)

    for slot in (1, 4, 5, 7, 8):
        arrived(kb, slot, k_recv)
    loop(9, scores)
    for slot in (1, 4, 5, 7, 8):
        arrived(vb, slot, v_recv)
    loop(9, weights)
    for n, cols in heads:
        lse[0, n : n + 1] = top[n] + jnp.log(total[n]) * LOG2E
    start("lse", 2, 3, 6, 1)
    for n, cols in heads:
        inverse = 1.0 / total[n]
        total[n] = inverse
        back = db[0, :, cols].astype(f32).T
        delta[0, n : n + 1] = jnp.sum(ot[n] * back, axis=0, keepdims=True) * inverse
    start("delta", 2, 3, 6, 1)

    def outward(c):
        chunk_arrived(6, c)
        chunk_copy(7, c).start()
        chunk_copy(8, c).start()

    loop(CHUNKS, outward)
    relay("lse", 6, 7, 8)
    relay("delta", 6, 7, 8)
    relay("q", 2, 4)
    relay("q", 3, 5)

    dqt[...] = jnp.zeros(dqt.shape, f32)

    def query_side(j):
        for n, cols in heads:
            dp = dot_nt(vb[j, :, cols], db[0, :, cols])
            ds = (pq[j, n].astype(f32) * (dp - delta[0, n : n + 1])).astype(bf16)
            dqt[n] += dot_tn(kb[j, :, cols], ds)

    loop(9, query_side)
    for n, cols in heads:
        dq_out[0, 0, :, cols] = (dqt[n] * (total[n] * SCALING)).T.astype(bf16)

    relay("lse", 2, 4)
    relay("lse", 3, 5)
    for slot in (1, 4, 5, 7, 8):
        arrived(qb, slot, q_recv)
    for slot in (1, 4, 5, 7, 8):
        arrived(lse, slot, lse_recv)

    def key_weights(j):
        bias = biases[1, j]
        for n, cols in heads:
            s = dot_nt(kb[0, :, cols], qb[j, :, cols]) * (SCALING * LOG2E) + bias
            pk[j, n] = jnp.exp2(s - lse[j, n : n + 1]).astype(bf16)

    loop(9, key_weights)

    def sideways(c):
        chunk_arrived(2, c)
        chunk_copy(4, c).start()
        chunk_arrived(3, c)
        chunk_copy(5, c).start()

    loop(CHUNKS, sideways)
    relay("delta", 2, 4)
    relay("delta", 3, 5)
    for slot in (1, 4, 5, 7, 8):
        arrived(delta, slot, delta_recv)
        loop(CHUNKS, functools.partial(chunk_arrived, slot))

    dk[...] = jnp.zeros(dk.shape, f32)
    dv[...] = jnp.zeros(dv.shape, f32)

    def key_side(j):
        for n, cols in heads:
            dp = dot_nt(vb[0, :, cols], db[j, :, cols])
            p = pk[j, n]
            ds = (p.astype(f32) * (dp - delta[j, n : n + 1])).astype(bf16)
            dv[n] += dot_nn(p, db[j, :, cols])
            dk[n] += dot_nn(ds, qb[j, :, cols])

    loop(9, key_side)
    for n, cols in heads:
        dk_out[0, 0, :, cols] = (dk[n] * SCALING).astype(bf16)
        dv_out[0, 0, :, cols] = dv[n].astype(bf16)

    for slot in range(1, 9):
        for name in tiles:
            buf, send, recv = tiles[name]
            tile_copy(buf, slot, send, recv).wait_send()
        for c in range(CHUNKS):
            chunk_copy(slot, c).wait_send()
    for kind in range(7):
        for c in range(CHUNKS):
            rs_copy(kind, c).wait_send()


def solution(mesh):
    frames = mesh.shape["tm"]
    rows_of_tiles = mesh.shape["height"]
    dma = pltpu.SemaphoreType.DMA

    def body(grad_output, out_weight, queries, key_states, value_states, window):
        shape = jax.ShapeDtypeStruct((1, 1, TILE, FEAT), bf16)
        anywhere = pl.BlockSpec(memory_space=pl.ANY)
        tile = (9, TILE, FEAT)
        return pl.pallas_call(
            functools.partial(kernel, frames, rows_of_tiles),
            out_shape=(shape, shape, shape),
            in_specs=[anywhere] * 5 + [pl.BlockSpec(memory_space=pltpu.SMEM)],
            out_specs=[pl.BlockSpec(memory_space=pltpu.VMEM)] * 3,
            scratch_shapes=[
                pltpu.VMEM(grad_output.shape[2:], bf16),
                pltpu.VMEM(out_weight.shape, bf16),
                pltpu.VMEM(tile, bf16),
                pltpu.VMEM(tile, bf16),
                pltpu.VMEM(tile, bf16),
                pltpu.VMEM(tile, bf16),
                pltpu.VMEM((9, 8, TILE), f32),
                pltpu.VMEM((9, 8, TILE), f32),
                pltpu.VMEM((9, HEADS_HERE, TILE, TILE), f32),
                pltpu.VMEM((9, HEADS_HERE, TILE, TILE), bf16),
                pltpu.VMEM((9, HEADS_HERE, TILE, TILE), bf16),
                pltpu.VMEM((HEADS_HERE, 1, TILE), f32),
                pltpu.VMEM((HEADS_HERE, 1, TILE), f32),
                pltpu.VMEM((HEADS_HERE, HD, TILE), f32),
                pltpu.VMEM((HEADS_HERE, HD, TILE), f32),
                pltpu.VMEM((HEADS_HERE, TILE, HD), f32),
                pltpu.VMEM((HEADS_HERE, TILE, HD), f32),
                pltpu.VMEM((2, TILE, FEAT), f32),
                pltpu.VMEM((7, TILE, FEAT), bf16),
                pltpu.VMEM((7, TILE, FEAT), bf16),
                pltpu.SMEM((2, 9), f32),
                dma((5,)),
                dma((9,)),
                dma((9,)),
                dma((9,)),
                dma((9,)),
                dma((9,)),
                dma((9,)),
                dma((9, CHUNKS)),
                dma((9, CHUNKS)),
                dma((9,)),
                dma((9,)),
                dma((9,)),
                dma((9,)),
                dma((7, CHUNKS)),
                dma((7, CHUNKS)),
            ],
            compiler_params=pltpu.CompilerParams(
                collective_id=0, has_side_effects=True, vmem_limit_bytes=60000 * 1024
            ),
        )(grad_output, out_weight, queries, key_states, value_states, window)

    spread = P("tm", "height", None, "heads")
    return jax.shard_map(
        body,
        mesh=mesh,
        in_specs=(spread, P(None, "heads"), spread, spread, spread, P()),
        out_specs=(spread, spread, spread),
        check_vma=False,
    )
```

```python
import functools

import jax
import jax.numpy as jnp
from jax import lax
from jax.experimental import pallas as pl
from jax.experimental.pallas import tpu as pltpu
from jax.sharding import PartitionSpec as P

HD = 128
TILE = 384
FEAT = 256
HEADS_HERE = 2
CHUNKS = 3
ROWS = TILE // CHUNKS
RING_X = 4
LOG2E = 1.4426950408889634
SCALING = HD ** (-0.5)
MESH = pl.DeviceIdType.MESH

FRAME = (0, 0, -1, 1, -1, 1, 0, -1, 1)
COLUMN = (0, 1, 0, 0, 1, 1, 2, 2, 2)
SOURCE = {1: 0, 2: 0, 3: 0, 6: 0, 4: 2, 5: 3, 7: 6, 8: 6}
SOURCE_ALONG_Y = {**SOURCE, 7: 2, 8: 3}
BLOCKS = tuple(slice(i * HD, (i + 1) * HD) for i in range(TILE // HD))

f32 = jnp.float32
bf16 = jnp.bfloat16


def dot_nt(a, b):
    return lax.dot_general(a, b, (((1,), (1,)), ((), ())), preferred_element_type=f32)


def dot_tn(a, b):
    return lax.dot_general(a, b, (((0,), (0,)), ((), ())), preferred_element_type=f32)


def dot_nn(a, b):
    return lax.dot_general(a, b, (((1,), (0,)), ((), ())), preferred_element_type=f32)


def loop(first, last, body):
    def step(index, carry):
        body(index)
        return carry

    lax.fori_loop(first, last, step, 0)


def when(condition, action):
    if condition is None:
        action()
    else:
        pl.when(condition)(action)


def spread(column):
    return jnp.broadcast_to(column, (TILE, HD))


def kernel(
    frames,
    rows_of_tiles,
    go_hbm,
    w_hbm,
    q_hbm,
    k_hbm,
    v_hbm,
    win,
    dq_out,
    dk_out,
    dv_out,
    go,
    w,
    kb,
    vb,
    qb,
    db,
    stats,
    sbuf,
    pq,
    top,
    total,
    mean,
    out,
    dq,
    dk,
    dv,
    own,
    rs_send,
    rs_recv,
    windows,
    biases,
    load_sem,
    k_send,
    k_recv,
    v_send,
    v_recv,
    q_send,
    q_recv,
    d_send,
    d_recv,
    stats_send,
    stats_recv,
    rs_ssem,
    rs_rsem,
):
    t = lax.axis_index("tm")
    h = lax.axis_index("height")
    g = lax.axis_index("heads")
    x = g // 2
    yl = g % 2
    odd = h % 2
    before = t > 0
    after = t < frames - 1
    beside = (h > 0) & (h < rows_of_tiles - 1)
    partner = {"height": h + 1 - 2 * odd}
    outer = {"height": (h + 2 * odd - 1 + rows_of_tiles) % rows_of_tiles}
    t_next = {"tm": (t + 1) % frames}
    t_prev = {"tm": (t + frames - 1) % frames}
    x_next = {"heads": ((x + 1) % RING_X) * 2 + yl}
    x_prev = {"heads": ((x + RING_X - 1) % RING_X) * 2 + yl}
    y_other = {"heads": x * 2 + 1 - yl}
    has = {2: before, 3: after, 4: before, 5: after, 6: beside, 7: before & beside, 8: after & beside}
    along_z = {1: partner, 4: partner, 5: partner, 2: t_next, 7: t_next, 3: t_prev, 8: t_prev, 6: outer}
    sends_z = {4: before, 5: after, 2: after, 7: after & beside, 3: before, 8: before & beside, 6: beside}
    along_y = {**along_z, 7: outer, 8: outer}
    sends_y = {**sends_z, 7: before & beside, 8: after & beside}

    barrier = pltpu.get_barrier_semaphore()

    def greet(peer):
        pl.semaphore_signal(barrier, inc=1, device_id=peer, device_id_type=MESH)

    for peer in (partner, x_next, x_prev, y_other):
        greet(peer)
    for condition, peer in ((before, t_prev), (after, t_next), (beside, outer)):
        when(condition, functools.partial(greet, peer))

    loads = [
        pltpu.make_async_copy(src, dst, load_sem.at[i])
        for i, (src, dst) in enumerate(
            (
                (k_hbm.at[0, 0], kb.at[0]),
                (v_hbm.at[0, 0], vb.at[0]),
                (go_hbm.at[0, 0], go),
                (w_hbm, w),
                (q_hbm.at[0, 0], qb.at[0]),
            )
        )
    ]
    sign = 1 - 2 * odd
    places = [(FRAME[slot], (0, sign, -sign)[COLUMN[slot]]) for slot in range(9)]
    loads += [
        pltpu.make_async_copy(
            win.at[(t + a + frames) % frames, (h + b + rows_of_tiles) % rows_of_tiles],
            windows.at[slot],
            load_sem.at[5 + slot],
        )
        for slot, (a, b) in enumerate(places)
    ]
    for load in loads:
        load.start()

    def chunk_rows(c):
        return pl.ds(pl.multiple_of(c * ROWS, ROWS), ROWS)

    def tile_copy(name, slot):
        buf, send, recv, source, target, _ = tiles[name]
        return pltpu.make_async_remote_copy(
            src_ref=buf.at[source[slot]],
            dst_ref=buf.at[slot],
            send_sem=send.at[slot],
            recv_sem=recv.at[slot],
            device_id=target[slot],
            device_id_type=MESH,
        )

    def chunk_copy(slot, c):
        rows = chunk_rows(c)
        return pltpu.make_async_remote_copy(
            src_ref=db.at[SOURCE[slot], rows],
            dst_ref=db.at[slot, rows],
            send_sem=d_send.at[slot, c],
            recv_sem=d_recv.at[slot, c],
            device_id=along_z[slot],
            device_id_type=MESH,
        )

    def rs_copy(kind, c):
        rows = chunk_rows(c)
        return pltpu.make_async_remote_copy(
            src_ref=rs_send.at[kind, rows],
            dst_ref=rs_recv.at[kind, rows],
            send_sem=rs_ssem.at[kind, c],
            recv_sem=rs_rsem.at[kind, c],
            device_id=(x_next, x_prev, x_next, x_next, x_prev, x_prev, y_other)[kind],
            device_id_type=MESH,
        )

    def landed(piece, semaphore):
        pltpu.make_async_copy(piece, piece, semaphore).wait()

    def rs_arrived(kind, c):
        landed(rs_recv.at[kind, chunk_rows(c)], rs_rsem.at[kind, c])

    tiles = {
        "k": (kb, k_send, k_recv, SOURCE, along_z, sends_z),
        "v": (vb, v_send, v_recv, SOURCE, along_z, sends_z),
        "q": (qb, q_send, q_recv, SOURCE_ALONG_Y, along_y, sends_y),
        "stats": (stats, stats_send, stats_recv, SOURCE, along_z, sends_z),
    }

    def arrived(name, *slots):
        buf, recv = tiles[name][0], tiles[name][2]
        for slot in slots:
            when(has.get(slot), lambda slot=slot: landed(buf.at[slot], recv.at[slot]))

    def start(name, *slots):
        for slot in slots:
            when(tiles[name][5].get(slot), lambda slot=slot: tile_copy(name, slot).start())

    def chunk_arrived(slot, c):
        when(has.get(slot), lambda: landed(db.at[slot, chunk_rows(c)], d_recv.at[slot, c]))

    def chunk_start(c, *slots):
        for slot in slots:
            when(sends_z.get(slot), lambda slot=slot: chunk_copy(slot, c).start())

    def present(j):
        earlier = (j == 2) | (j == 4) | (j == 7)
        later = (j == 3) | (j == 5) | (j == 8)
        missing = (earlier & (t == 0)) | (later & (t == frames - 1))
        missing = missing | ((j >= 6) & ((h == 0) | (h == rows_of_tiles - 1)))
        return jnp.logical_not(missing)

    def over(first, last, body):
        loop(first, last, lambda j: pl.when(present(j))(lambda: body(j)))

    def partial(column, half, c):
        block = (2 * ((x + column) % RING_X) + (yl if half == 0 else 1 - yl)) * FEAT
        return dot_nt(go[chunk_rows(c), :], w[pl.ds(pl.multiple_of(block, FEAT), FEAT), :])

    def far(c):
        rs_send[0, chunk_rows(c), :] = partial(2, 0, c).astype(bf16)
        rs_send[1, chunk_rows(c), :] = partial(2, 1, c).astype(bf16)

    def near(c):
        rs_send[3, chunk_rows(c), :] = partial(1, 1, c).astype(bf16)
        rs_send[4, chunk_rows(c), :] = partial(3, 0, c).astype(bf16)
        own[0, chunk_rows(c), :] = partial(0, 0, c)
        own[1, chunk_rows(c), :] = partial(0, 1, c)

    loads[2].wait()
    loads[3].wait()
    loop(0, CHUNKS, far)
    loads[0].wait()
    loads[1].wait()

    pl.semaphore_wait(barrier, 4 + sum(jnp.where(condition, 1, 0) for condition in (before, after, beside)))

    start("k", 2, 3, 6, 1)

    def far_send(c):
        rs_copy(0, c).start()
        rs_copy(1, c).start()

    loop(0, CHUNKS, far_send)
    start("v", 2, 3, 6, 1)
    loads[4].wait()
    start("q", 6, 1)
    loop(0, CHUNKS, near)

    for slot, (a, b) in enumerate(places):
        loads[5 + slot].wait()
    for slot, (a, b) in enumerate(places):
        seen = windows[0, 0, 9 * (a + 1) + 3 * (b + 1) + 1]
        biases[0, slot] = (seen.astype(f32) - 1.0) * 1e30
        seen = windows[slot, 0, 9 * (1 - a) + 3 * (1 - b) + 1]
        biases[1, slot] = (seen.astype(f32) - 1.0) * 1e30

    heads = [(n, slice(n * HD, (n + 1) * HD)) for n in range(HEADS_HERE)]
    top[...] = jnp.full(top.shape, -1e30, f32)
    for ref in (total, out, dq, dk, dv):
        ref[...] = jnp.zeros(ref.shape, f32)

    def combine(c):
        rs_arrived(0, c)
        rs_send[2, chunk_rows(c), :] = (partial(1, 0, c) + rs_recv[0, chunk_rows(c), :].astype(f32)).astype(bf16)
        rs_copy(2, c).start()
        rs_arrived(1, c)
        rs_send[5, chunk_rows(c), :] = (partial(3, 1, c) + rs_recv[1, chunk_rows(c), :].astype(f32)).astype(bf16)
        rs_copy(5, c).start()
        rs_copy(3, c).start()
        rs_copy(4, c).start()

    loop(0, CHUNKS, combine)

    def scores(j):
        bias = biases[0, j]
        for n, cols in heads:
            s = dot_nt(qb[0, :, cols], kb[j, :, cols]) * (SCALING * LOG2E) + bias
            sbuf[j, n] = s
            highest = top[n]
            for block in BLOCKS:
                highest = jnp.maximum(highest, s[:, block])
            top[n] = highest

    def weights(j):
        for n, cols in heads:
            summed = total[n]
            for block in BLOCKS:
                p = jnp.exp2(sbuf[j, n, :, block] - top[n])
                summed = summed + p
                pq[j, n, :, block] = p.astype(bf16)
            total[n] = summed
            out[n] += dot_nn(pq[j, n], vb[j, :, cols])

    def cross(c):
        rs_arrived(3, c)
        rs_arrived(5, c)
        rs_send[6, chunk_rows(c), :] = (
            own[1, chunk_rows(c), :]
            + rs_recv[3, chunk_rows(c), :].astype(f32)
            + rs_recv[5, chunk_rows(c), :].astype(f32)
        ).astype(bf16)
        rs_copy(6, c).start()

    def settle(c):
        rs_arrived(2, c)
        rs_arrived(4, c)
        summed = (
            own[0, chunk_rows(c), :]
            + rs_recv[2, chunk_rows(c), :].astype(f32)
            + rs_recv[4, chunk_rows(c), :].astype(f32)
        )
        rs_arrived(6, c)
        db[0, chunk_rows(c), :] = (summed + rs_recv[6, chunk_rows(c), :].astype(f32)).astype(bf16)
        chunk_start(c, 2, 3, 6, 1)

    arrived("k", 6, 2, 3)
    start("k", 7, 8, 4, 5)
    arrived("k", 1)
    over(0, 4, scores)
    cross(0)
    arrived("k", 4, 5)
    over(4, 7, scores)
    arrived("v", 6, 2, 3)
    start("v", 7, 8, 4, 5)
    start("q", 2, 3)
    cross(1)
    settle(0)
    cross(2)
    settle(1)
    settle(2)
    arrived("k", 7, 8)
    over(7, 9, scores)
    for n, cols in heads:
        top[n] = spread(jnp.max(top[n], axis=1, keepdims=True))
    arrived("v", 1, 4, 5)
    over(0, 7, weights)
    arrived("v", 7, 8)
    over(7, 9, weights)

    columns = []
    for n, cols in heads:
        summed = spread(jnp.sum(total[n], axis=1, keepdims=True))
        inverse = 1.0 / summed
        total[n] = inverse
        columns.append(top[n] + jnp.log(summed) * LOG2E)
        slope = jnp.sum(out[n] * db[0, :, cols].astype(f32), axis=1, keepdims=True)
        mean[n] = spread(slope) * inverse
        columns.append(mean[n])
    lane = lax.broadcasted_iota(jnp.int32, (TILE, HD), 1)
    packed = columns[0]
    for i in range(1, 4):
        packed = jnp.where(lane == i, columns[i], packed)
    stats[0] = packed.T[:8]
    start("stats", 2, 3, 6, 1)

    def outward(c):
        chunk_arrived(6, c)
        chunk_start(c, 7, 8)

    loop(0, CHUNKS, outward)

    def query_side(j):
        for n, cols in heads:
            dp = dot_nt(db[0, :, cols], vb[j, :, cols])
            ds = jnp.concatenate(
                [(pq[j, n, :, block].astype(f32) * (dp[:, block] - mean[n])).astype(bf16) for block in BLOCKS], axis=1
            )
            dq[n] += dot_nn(ds, kb[j, :, cols])

    over(0, 3, query_side)
    arrived("q", 2, 3)
    start("q", 7, 8, 4, 5)
    arrived("stats", 6, 2, 3)
    start("stats", 7, 8, 4, 5)
    over(3, 9, query_side)

    def key_side(j):
        bias = biases[1, j]
        for n, cols in heads:
            s = dot_nt(kb[0, :, cols], qb[j, :, cols]) * (SCALING * LOG2E) + bias
            p = jnp.exp2(s - stats[j, 2 * n : 2 * n + 1])
            low = p.astype(bf16)
            dv[n] += dot_nn(low, db[j, :, cols])
            dp = dot_nt(vb[0, :, cols], db[j, :, cols])
            ds = (p * (dp - stats[j, 2 * n + 1 : 2 * n + 2])).astype(bf16)
            dk[n] += dot_nn(ds, qb[j, :, cols])

    def sideways(c):
        chunk_arrived(2, c)
        chunk_start(c, 4)
        chunk_arrived(3, c)
        chunk_start(c, 5)

    def ready(*slots):
        arrived("q", *[slot for slot in slots if slot not in (2, 3)])
        arrived("stats", *[slot for slot in slots if slot not in (2, 3, 6)])
        for slot in slots:
            if slot not in (2, 3, 6):
                loop(0, CHUNKS, functools.partial(chunk_arrived, slot))

    ready(1)
    over(0, 2, key_side)
    loop(0, CHUNKS, sideways)
    for n, cols in heads:
        dq_out[0, 0, :, cols] = (dq[n] * (total[n] * SCALING)).astype(bf16)
    ready(6, 4, 5)
    over(2, 7, key_side)
    ready(7, 8)
    over(7, 9, key_side)
    for n, cols in heads:
        dk_out[0, 0, :, cols] = (dk[n] * SCALING).astype(bf16)
        dv_out[0, 0, :, cols] = dv[n].astype(bf16)

    for slot in range(1, 9):
        for name in tiles:
            when(tiles[name][5].get(slot), lambda name=name, slot=slot: tile_copy(name, slot).wait_send())
        when(
            sends_z.get(slot),
            lambda slot=slot: loop(0, CHUNKS, lambda c: chunk_copy(slot, c).wait_send()),
        )
    for kind in range(7):
        loop(0, CHUNKS, lambda c, kind=kind: rs_copy(kind, c).wait_send())


def deliver(*refs):
    copies = [pltpu.make_async_copy(refs[i], refs[3 + i], refs[6].at[i]) for i in range(3)]
    for copy in copies:
        copy.start()
    for copy in copies:
        copy.wait()


def solution(mesh):
    frames = mesh.shape["tm"]
    rows_of_tiles = mesh.shape["height"]
    dma = pltpu.SemaphoreType.DMA

    def body(grad_output, out_weight, queries, key_states, value_states, window):
        shape = jax.ShapeDtypeStruct((1, 1, TILE, FEAT), bf16)
        hbm = pl.BlockSpec(memory_space=pltpu.HBM)
        vmem = pl.BlockSpec(memory_space=pltpu.VMEM)
        tile = (9, TILE, FEAT)
        column = (HEADS_HERE, TILE, HD)
        results = pl.pallas_call(
            functools.partial(kernel, frames, rows_of_tiles),
            out_shape=(shape, shape, shape),
            in_specs=[hbm] * 6,
            out_specs=[vmem] * 3,
            scratch_shapes=[
                pltpu.VMEM(grad_output.shape[2:], bf16),
                pltpu.VMEM(out_weight.shape, bf16),
                pltpu.VMEM(tile, bf16),
                pltpu.VMEM(tile, bf16),
                pltpu.VMEM(tile, bf16),
                pltpu.VMEM(tile, bf16),
                pltpu.VMEM((9, 8, TILE), f32),
                pltpu.VMEM((9, HEADS_HERE, TILE, TILE), f32),
                pltpu.VMEM((9, HEADS_HERE, TILE, TILE), bf16),
                pltpu.VMEM(column, f32),
                pltpu.VMEM(column, f32),
                pltpu.VMEM(column, f32),
                pltpu.VMEM(column, f32),
                pltpu.VMEM(column, f32),
                pltpu.VMEM(column, f32),
                pltpu.VMEM(column, f32),
                pltpu.VMEM((2, TILE, FEAT), f32),
                pltpu.VMEM((7, TILE, FEAT), bf16),
                pltpu.VMEM((7, TILE, FEAT), bf16),
                pltpu.SMEM((9, 1, 27), jnp.int32),
                pltpu.SMEM((2, 9), f32),
                dma((14,)),
                dma((9,)),
                dma((9,)),
                dma((9,)),
                dma((9,)),
                dma((9,)),
                dma((9,)),
                dma((9, CHUNKS)),
                dma((9, CHUNKS)),
                dma((9,)),
                dma((9,)),
                dma((7, CHUNKS)),
                dma((7, CHUNKS)),
            ],
            compiler_params=pltpu.CompilerParams(
                collective_id=0, has_side_effects=True, vmem_limit_bytes=54400 * 1024
            ),
        )(grad_output, out_weight, queries, key_states, value_states, window)
        return pl.pallas_call(
            deliver,
            out_shape=(shape, shape, shape),
            in_specs=[vmem] * 3,
            out_specs=[hbm] * 3,
            scratch_shapes=[dma((3,))],
            compiler_params=pltpu.CompilerParams(vmem_limit_bytes=4096 * 1024),
        )(*results)

    split = P("tm", "height", None, "heads")
    return jax.shard_map(
        body,
        mesh=mesh,
        in_specs=(split, P(None, "heads"), split, split, split, P()),
        out_specs=(split, split, split),
        check_vma=False,
    )
```

```python
import functools

import jax
import jax.numpy as jnp
from jax import lax
from jax.experimental import pallas as pl
from jax.experimental.pallas import tpu as pltpu
from jax.sharding import PartitionSpec as P

HD = 128
TILE = 384
FEAT = 256
HEADS_HERE = 2
CHUNKS = 3
ROWS = TILE // CHUNKS
RING_X = 4
LOG2E = 1.4426950408889634
SCALING = HD ** (-0.5)
MESH = pl.DeviceIdType.MESH

FRAME = (0, 0, -1, 1, -1, 1, 0, -1, 1)
COLUMN = (0, 1, 0, 0, 1, 1, 2, 2, 2)
SOURCE = {1: 0, 2: 0, 3: 0, 6: 0, 4: 2, 5: 3, 7: 6, 8: 6}
SOURCE_STRAIGHT = {**SOURCE, 7: 0, 8: 0}
BLOCKS = tuple(slice(i * HD, (i + 1) * HD) for i in range(TILE // HD))

f32 = jnp.float32
bf16 = jnp.bfloat16


def dot_nt(a, b):
    return lax.dot_general(a, b, (((1,), (1,)), ((), ())), preferred_element_type=f32)


def dot_tn(a, b):
    return lax.dot_general(a, b, (((0,), (0,)), ((), ())), preferred_element_type=f32)


def dot_nn(a, b):
    return lax.dot_general(a, b, (((1,), (0,)), ((), ())), preferred_element_type=f32)


def loop(first, last, body):
    def step(index, carry):
        body(index)
        return carry

    lax.fori_loop(first, last, step, 0)


def when(condition, action):
    if condition is None:
        action()
    else:
        pl.when(condition)(action)


def spread(column):
    return jnp.broadcast_to(column, (TILE, HD))


def kernel(
    frames,
    rows_of_tiles,
    go_hbm,
    w_hbm,
    q_hbm,
    k_hbm,
    v_hbm,
    win,
    dq_out,
    dk_out,
    dv_out,
    go,
    w,
    kb,
    vb,
    qb,
    db,
    stats,
    sbuf,
    pq,
    top,
    total,
    mean,
    out,
    dq,
    dk,
    dv,
    own,
    rs_send,
    rs_recv,
    windows,
    biases,
    load_sem,
    k_send,
    k_recv,
    v_send,
    v_recv,
    q_send,
    q_recv,
    d_send,
    d_recv,
    stats_send,
    stats_recv,
    rs_ssem,
    rs_rsem,
):
    t = lax.axis_index("tm")
    h = lax.axis_index("height")
    g = lax.axis_index("heads")
    x = g // 2
    yl = g % 2
    odd = h % 2
    before = t > 0
    after = t < frames - 1
    beside = (h > 0) & (h < rows_of_tiles - 1)
    partner = {"height": h + 1 - 2 * odd}
    outer = {"height": (h + 2 * odd - 1 + rows_of_tiles) % rows_of_tiles}
    t_next = {"tm": (t + 1) % frames}
    t_prev = {"tm": (t + frames - 1) % frames}
    x_next = {"heads": ((x + 1) % RING_X) * 2 + yl}
    x_prev = {"heads": ((x + RING_X - 1) % RING_X) * 2 + yl}
    y_other = {"heads": x * 2 + 1 - yl}
    has = {2: before, 3: after, 4: before, 5: after, 6: beside, 7: before & beside, 8: after & beside}
    along_z = {1: partner, 4: partner, 5: partner, 2: t_next, 7: t_next, 3: t_prev, 8: t_prev, 6: outer}
    sends_z = {4: before, 5: after, 2: after, 7: after & beside, 3: before, 8: before & beside, 6: beside}
    straight = {**along_z, 7: {**t_next, **outer}, 8: {**t_prev, **outer}}

    barrier = pltpu.get_barrier_semaphore()

    def greet(peer):
        pl.semaphore_signal(barrier, inc=1, device_id=peer, device_id_type=MESH)

    for peer in (partner, x_next, x_prev, y_other):
        greet(peer)
    neighbours = ((before, t_prev), (after, t_next), (beside, outer), (sends_z[7], straight[7]), (sends_z[8], straight[8]))
    for condition, peer in neighbours:
        when(condition, functools.partial(greet, peer))

    loads = [
        pltpu.make_async_copy(src, dst, load_sem.at[i])
        for i, (src, dst) in enumerate(
            (
                (k_hbm.at[0, 0], kb.at[0]),
                (v_hbm.at[0, 0], vb.at[0]),
                (go_hbm.at[0, 0], go),
                (w_hbm, w),
                (q_hbm.at[0, 0], qb.at[0]),
            )
        )
    ]
    sign = 1 - 2 * odd
    places = [(FRAME[slot], (0, sign, -sign)[COLUMN[slot]]) for slot in range(9)]
    loads += [
        pltpu.make_async_copy(
            win.at[(t + a + frames) % frames, (h + b + rows_of_tiles) % rows_of_tiles],
            windows.at[slot],
            load_sem.at[5 + slot],
        )
        for slot, (a, b) in enumerate(places)
    ]
    for load in loads:
        load.start()

    def chunk_rows(c):
        return pl.ds(pl.multiple_of(c * ROWS, ROWS), ROWS)

    def tile_copy(name, slot):
        buf, send, recv, source, target, _ = tiles[name]
        return pltpu.make_async_remote_copy(
            src_ref=buf.at[source[slot]],
            dst_ref=buf.at[slot],
            send_sem=send.at[slot],
            recv_sem=recv.at[slot],
            device_id=target[slot],
            device_id_type=MESH,
        )

    def chunk_copy(slot, c):
        rows = chunk_rows(c)
        return pltpu.make_async_remote_copy(
            src_ref=db.at[SOURCE_STRAIGHT[slot], rows],
            dst_ref=db.at[slot, rows],
            send_sem=d_send.at[slot, c],
            recv_sem=d_recv.at[slot, c],
            device_id=straight[slot],
            device_id_type=MESH,
        )

    def rs_copy(kind, c):
        rows = chunk_rows(c)
        return pltpu.make_async_remote_copy(
            src_ref=rs_send.at[kind, rows],
            dst_ref=rs_recv.at[kind, rows],
            send_sem=rs_ssem.at[kind, c],
            recv_sem=rs_rsem.at[kind, c],
            device_id=(x_next, x_prev, x_next, x_next, x_prev, x_prev, y_other)[kind],
            device_id_type=MESH,
        )

    def landed(piece, semaphore):
        pltpu.make_async_copy(piece, piece, semaphore).wait()

    def rs_arrived(kind, c):
        landed(rs_recv.at[kind, chunk_rows(c)], rs_rsem.at[kind, c])

    tiles = {
        "k": (kb, k_send, k_recv, SOURCE, along_z, sends_z),
        "v": (vb, v_send, v_recv, SOURCE, along_z, sends_z),
        "q": (qb, q_send, q_recv, SOURCE, along_z, sends_z),
        "stats": (stats, stats_send, stats_recv, SOURCE_STRAIGHT, straight, sends_z),
    }

    def arrived(name, *slots):
        buf, recv = tiles[name][0], tiles[name][2]
        for slot in slots:
            when(has.get(slot), lambda slot=slot: landed(buf.at[slot], recv.at[slot]))

    def start(name, *slots):
        for slot in slots:
            when(tiles[name][5].get(slot), lambda slot=slot: tile_copy(name, slot).start())

    def chunk_arrived(slot, c):
        when(has.get(slot), lambda: landed(db.at[slot, chunk_rows(c)], d_recv.at[slot, c]))

    def chunk_start(c, *slots):
        for slot in slots:
            when(sends_z.get(slot), lambda slot=slot: chunk_copy(slot, c).start())

    def present(j):
        earlier = (j == 2) | (j == 4) | (j == 7)
        later = (j == 3) | (j == 5) | (j == 8)
        missing = (earlier & (t == 0)) | (later & (t == frames - 1))
        missing = missing | ((j >= 6) & ((h == 0) | (h == rows_of_tiles - 1)))
        return jnp.logical_not(missing)

    def over(first, last, body):
        loop(first, last, lambda j: pl.when(present(j))(lambda: body(j)))

    def partial(column, half, c):
        block = (2 * ((x + column) % RING_X) + (yl if half == 0 else 1 - yl)) * FEAT
        return dot_nt(go[chunk_rows(c), :], w[pl.ds(pl.multiple_of(block, FEAT), FEAT), :])

    def far(c):
        rs_send[0, chunk_rows(c), :] = partial(2, 0, c).astype(bf16)
        rs_send[1, chunk_rows(c), :] = partial(2, 1, c).astype(bf16)

    def near(c):
        rs_send[3, chunk_rows(c), :] = partial(1, 1, c).astype(bf16)
        rs_send[4, chunk_rows(c), :] = partial(3, 0, c).astype(bf16)
        own[0, chunk_rows(c), :] = partial(0, 0, c)
        own[1, chunk_rows(c), :] = partial(0, 1, c)

    loads[2].wait()
    loads[3].wait()
    loop(0, CHUNKS, far)
    loads[0].wait()
    loads[1].wait()

    pl.semaphore_wait(barrier, 4 + sum(jnp.where(condition, 1, 0) for condition, _ in neighbours))

    start("k", 2, 3, 6, 1)

    def far_send(c):
        rs_copy(0, c).start()
        rs_copy(1, c).start()

    loop(0, CHUNKS, far_send)
    start("v", 2, 3, 6, 1)
    loads[4].wait()
    start("q", 6, 1)
    loop(0, CHUNKS, near)

    for slot, (a, b) in enumerate(places):
        loads[5 + slot].wait()
    for slot, (a, b) in enumerate(places):
        seen = windows[0, 0, 9 * (a + 1) + 3 * (b + 1) + 1]
        biases[0, slot] = (seen.astype(f32) - 1.0) * 1e30
        seen = windows[slot, 0, 9 * (1 - a) + 3 * (1 - b) + 1]
        biases[1, slot] = (seen.astype(f32) - 1.0) * 1e30

    heads = [(n, slice(n * HD, (n + 1) * HD)) for n in range(HEADS_HERE)]
    top[...] = jnp.full(top.shape, -1e30, f32)
    for ref in (total, out, dq, dk, dv):
        ref[...] = jnp.zeros(ref.shape, f32)

    def combine(c):
        rs_arrived(0, c)
        rs_send[2, chunk_rows(c), :] = (partial(1, 0, c) + rs_recv[0, chunk_rows(c), :].astype(f32)).astype(bf16)
        rs_copy(2, c).start()
        rs_arrived(1, c)
        rs_send[5, chunk_rows(c), :] = (partial(3, 1, c) + rs_recv[1, chunk_rows(c), :].astype(f32)).astype(bf16)
        rs_copy(5, c).start()
        rs_copy(3, c).start()
        rs_copy(4, c).start()

    loop(0, CHUNKS, combine)

    def scores(j):
        bias = biases[0, j]
        for n, cols in heads:
            s = dot_nt(qb[0, :, cols], kb[j, :, cols]) * (SCALING * LOG2E) + bias
            sbuf[j, n] = s
            highest = top[n]
            for block in BLOCKS:
                highest = jnp.maximum(highest, s[:, block])
            top[n] = highest

    def weights(j):
        for n, cols in heads:
            summed = total[n]
            for block in BLOCKS:
                p = jnp.exp2(sbuf[j, n, :, block] - top[n])
                summed = summed + p
                pq[j, n, :, block] = p.astype(bf16)
            total[n] = summed
            out[n] += dot_nn(pq[j, n], vb[j, :, cols])

    def cross(c):
        rs_arrived(3, c)
        rs_arrived(5, c)
        rs_send[6, chunk_rows(c), :] = (
            own[1, chunk_rows(c), :]
            + rs_recv[3, chunk_rows(c), :].astype(f32)
            + rs_recv[5, chunk_rows(c), :].astype(f32)
        ).astype(bf16)
        rs_copy(6, c).start()

    def settle(c):
        rs_arrived(2, c)
        rs_arrived(4, c)
        summed = (
            own[0, chunk_rows(c), :]
            + rs_recv[2, chunk_rows(c), :].astype(f32)
            + rs_recv[4, chunk_rows(c), :].astype(f32)
        )
        rs_arrived(6, c)
        db[0, chunk_rows(c), :] = (summed + rs_recv[6, chunk_rows(c), :].astype(f32)).astype(bf16)
        chunk_start(c, 2, 3, 6, 1)

    arrived("k", 6, 2, 3)
    start("k", 7, 8, 4, 5)
    arrived("k", 1)
    over(0, 4, scores)
    cross(0)
    arrived("k", 4, 5)
    over(4, 7, scores)
    arrived("v", 6, 2, 3)
    start("v", 7, 8, 4, 5)
    start("q", 2, 3)
    cross(1)
    settle(0)
    cross(2)
    settle(1)
    settle(2)
    arrived("k", 7, 8)
    over(7, 9, scores)
    for n, cols in heads:
        top[n] = spread(jnp.max(top[n], axis=1, keepdims=True))
    arrived("v", 1, 4, 5)
    over(0, 7, weights)
    arrived("v", 7, 8)
    over(7, 9, weights)

    columns = []
    for n, cols in heads:
        summed = spread(jnp.sum(total[n], axis=1, keepdims=True))
        inverse = 1.0 / summed
        total[n] = inverse
        columns.append(top[n] + jnp.log(summed) * LOG2E)
        slope = jnp.sum(out[n] * db[0, :, cols].astype(f32), axis=1, keepdims=True)
        mean[n] = spread(slope) * inverse
        columns.append(mean[n])
    lane = lax.broadcasted_iota(jnp.int32, (TILE, HD), 1)
    packed = columns[0]
    for i in range(1, 4):
        packed = jnp.where(lane == i, columns[i], packed)
    stats[0] = packed.T[:8]
    start("stats", 2, 3, 6, 1, 7, 8)
    arrived("q", 6)
    start("q", 7, 8)
    loop(0, CHUNKS, lambda c: chunk_start(c, 7, 8))

    def query_side(j):
        for n, cols in heads:
            dp = dot_nt(db[0, :, cols], vb[j, :, cols])
            ds = jnp.concatenate(
                [(pq[j, n, :, block].astype(f32) * (dp[:, block] - mean[n])).astype(bf16) for block in BLOCKS], axis=1
            )
            dq[n] += dot_nn(ds, kb[j, :, cols])

    over(0, 7, query_side)
    arrived("q", 2, 3)
    start("q", 4, 5)
    over(7, 9, query_side)

    def key_side(j):
        bias = biases[1, j]
        for n, cols in heads:
            s = dot_nt(kb[0, :, cols], qb[j, :, cols]) * (SCALING * LOG2E) + bias
            p = jnp.exp2(s - stats[j, 2 * n : 2 * n + 1])
            low = p.astype(bf16)
            dv[n] += dot_nn(low, db[j, :, cols])
            dp = dot_nt(vb[0, :, cols], db[j, :, cols])
            ds = (p * (dp - stats[j, 2 * n + 1 : 2 * n + 2])).astype(bf16)
            dk[n] += dot_nn(ds, qb[j, :, cols])

    def sideways(c):
        chunk_arrived(2, c)
        chunk_start(c, 4)
        chunk_arrived(3, c)
        chunk_start(c, 5)

    def ready(*slots):
        arrived("q", *[slot for slot in slots if slot != 6])
        arrived("stats", *slots)
        for slot in slots:
            loop(0, CHUNKS, functools.partial(chunk_arrived, slot))

    ready(1)
    over(0, 2, key_side)
    loop(0, CHUNKS, sideways)
    arrived("stats", 2, 3)
    start("stats", 4, 5)
    for n, cols in heads:
        dq_out[0, 0, :, cols] = (dq[n] * (total[n] * SCALING)).astype(bf16)
    ready(6, 4, 5)
    over(2, 7, key_side)
    ready(7, 8)
    over(7, 9, key_side)
    for n, cols in heads:
        dk_out[0, 0, :, cols] = (dk[n] * SCALING).astype(bf16)
        dv_out[0, 0, :, cols] = dv[n].astype(bf16)

    for slot in range(1, 9):
        for name in tiles:
            when(tiles[name][5].get(slot), lambda name=name, slot=slot: tile_copy(name, slot).wait_send())
        when(
            sends_z.get(slot),
            lambda slot=slot: loop(0, CHUNKS, lambda c: chunk_copy(slot, c).wait_send()),
        )
    for kind in range(7):
        loop(0, CHUNKS, lambda c, kind=kind: rs_copy(kind, c).wait_send())


def deliver(*refs):
    copies = [pltpu.make_async_copy(refs[i], refs[3 + i], refs[6].at[i]) for i in range(3)]
    for copy in copies:
        copy.start()
    for copy in copies:
        copy.wait()


def solution(mesh):
    frames = mesh.shape["tm"]
    rows_of_tiles = mesh.shape["height"]
    dma = pltpu.SemaphoreType.DMA

    def body(grad_output, out_weight, queries, key_states, value_states, window):
        shape = jax.ShapeDtypeStruct((1, 1, TILE, FEAT), bf16)
        hbm = pl.BlockSpec(memory_space=pltpu.HBM)
        vmem = pl.BlockSpec(memory_space=pltpu.VMEM)
        tile = (9, TILE, FEAT)
        column = (HEADS_HERE, TILE, HD)
        results = pl.pallas_call(
            functools.partial(kernel, frames, rows_of_tiles),
            out_shape=(shape, shape, shape),
            in_specs=[hbm] * 6,
            out_specs=[vmem] * 3,
            scratch_shapes=[
                pltpu.VMEM(grad_output.shape[2:], bf16),
                pltpu.VMEM(out_weight.shape, bf16),
                pltpu.VMEM(tile, bf16),
                pltpu.VMEM(tile, bf16),
                pltpu.VMEM(tile, bf16),
                pltpu.VMEM(tile, bf16),
                pltpu.VMEM((9, 8, TILE), f32),
                pltpu.VMEM((9, HEADS_HERE, TILE, TILE), f32),
                pltpu.VMEM((9, HEADS_HERE, TILE, TILE), bf16),
                pltpu.VMEM(column, f32),
                pltpu.VMEM(column, f32),
                pltpu.VMEM(column, f32),
                pltpu.VMEM(column, f32),
                pltpu.VMEM(column, f32),
                pltpu.VMEM(column, f32),
                pltpu.VMEM(column, f32),
                pltpu.VMEM((2, TILE, FEAT), f32),
                pltpu.VMEM((7, TILE, FEAT), bf16),
                pltpu.VMEM((7, TILE, FEAT), bf16),
                pltpu.SMEM((9, 1, 27), jnp.int32),
                pltpu.SMEM((2, 9), f32),
                dma((14,)),
                dma((9,)),
                dma((9,)),
                dma((9,)),
                dma((9,)),
                dma((9,)),
                dma((9,)),
                dma((9, CHUNKS)),
                dma((9, CHUNKS)),
                dma((9,)),
                dma((9,)),
                dma((7, CHUNKS)),
                dma((7, CHUNKS)),
            ],
            compiler_params=pltpu.CompilerParams(
                collective_id=0, has_side_effects=True, vmem_limit_bytes=54400 * 1024
            ),
        )(grad_output, out_weight, queries, key_states, value_states, window)
        return pl.pallas_call(
            deliver,
            out_shape=(shape, shape, shape),
            in_specs=[vmem] * 3,
            out_specs=[hbm] * 3,
            scratch_shapes=[dma((3,))],
            compiler_params=pltpu.CompilerParams(vmem_limit_bytes=4096 * 1024),
        )(*results)

    split = P("tm", "height", None, "heads")
    return jax.shard_map(
        body,
        mesh=mesh,
        in_specs=(split, P(None, "heads"), split, split, split, P()),
        out_specs=(split, split, split),
        check_vma=False,
    )
```

```python
import functools

import jax
import jax.numpy as jnp
from jax import lax
from jax.experimental import pallas as pl
from jax.experimental.pallas import tpu as pltpu
from jax.sharding import PartitionSpec as P

HD = 128
TILE = 384
FEAT = 256
HEADS_HERE = 2
CHUNKS = 3
ROWS = TILE // CHUNKS
RING_X = 4
LOG2E = 1.4426950408889634
SCALING = HD ** (-0.5)
MESH = pl.DeviceIdType.MESH

FRAME = (0, 0, -1, 1, -1, 1, 0, -1, 1)
COLUMN = (0, 1, 0, 0, 1, 1, 2, 2, 2)
SOURCE = {1: 0, 2: 0, 3: 0, 6: 0, 4: 2, 5: 3, 7: 6, 8: 6}
SOURCE_STRAIGHT = {**SOURCE, 7: 0, 8: 0}
BLOCKS = tuple(slice(i * HD, (i + 1) * HD) for i in range(TILE // HD))

f32 = jnp.float32
bf16 = jnp.bfloat16


def dot_nt(a, b):
    return lax.dot_general(a, b, (((1,), (1,)), ((), ())), preferred_element_type=f32)


def dot_tn(a, b):
    return lax.dot_general(a, b, (((0,), (0,)), ((), ())), preferred_element_type=f32)


def dot_nn(a, b):
    return lax.dot_general(a, b, (((1,), (0,)), ((), ())), preferred_element_type=f32)


def loop(first, last, body):
    def step(index, carry):
        body(index)
        return carry

    lax.fori_loop(first, last, step, 0)


def when(condition, action):
    if condition is None:
        action()
    else:
        pl.when(condition)(action)


def spread(column):
    return jnp.broadcast_to(column, (TILE, HD))


def kernel(
    frames,
    rows_of_tiles,
    go_hbm,
    w_hbm,
    q_hbm,
    k_hbm,
    v_hbm,
    win,
    dq_out,
    dk_out,
    dv_out,
    go,
    w,
    kb,
    vb,
    qb,
    db,
    stats,
    sbuf,
    pq,
    top,
    total,
    mean,
    out,
    dq,
    dk,
    dv,
    own,
    rs_send,
    rs_recv,
    windows,
    biases,
    load_sem,
    k_send,
    k_recv,
    v_send,
    v_recv,
    q_send,
    q_recv,
    d_send,
    d_recv,
    stats_send,
    stats_recv,
    rs_ssem,
    rs_rsem,
):
    t = lax.axis_index("tm")
    h = lax.axis_index("height")
    g = lax.axis_index("heads")
    x = g // 2
    yl = g % 2
    odd = h % 2
    before = t > 0
    after = t < frames - 1
    beside = (h > 0) & (h < rows_of_tiles - 1)
    partner = {"height": h + 1 - 2 * odd}
    outer = {"height": (h + 2 * odd - 1 + rows_of_tiles) % rows_of_tiles}
    t_next = {"tm": (t + 1) % frames}
    t_prev = {"tm": (t + frames - 1) % frames}
    x_next = {"heads": ((x + 1) % RING_X) * 2 + yl}
    x_prev = {"heads": ((x + RING_X - 1) % RING_X) * 2 + yl}
    y_other = {"heads": x * 2 + 1 - yl}
    has = {2: before, 3: after, 4: before, 5: after, 6: beside, 7: before & beside, 8: after & beside}
    along_z = {1: partner, 4: partner, 5: partner, 2: t_next, 7: t_next, 3: t_prev, 8: t_prev, 6: outer}
    sends_z = {4: before, 5: after, 2: after, 7: after & beside, 3: before, 8: before & beside, 6: beside}
    straight = {**along_z, 7: {**t_next, **outer}, 8: {**t_prev, **outer}}

    barrier = pltpu.get_barrier_semaphore()

    def greet(peer):
        pl.semaphore_signal(barrier, inc=1, device_id=peer, device_id_type=MESH)

    for peer in (partner, x_next, x_prev, y_other):
        greet(peer)
    neighbours = ((before, t_prev), (after, t_next), (beside, outer), (sends_z[7], straight[7]), (sends_z[8], straight[8]))
    for condition, peer in neighbours:
        when(condition, functools.partial(greet, peer))

    loads = [
        pltpu.make_async_copy(src, dst, load_sem.at[i])
        for i, (src, dst) in enumerate(
            (
                (k_hbm.at[0, 0], kb.at[0]),
                (v_hbm.at[0, 0], vb.at[0]),
                (go_hbm.at[0, 0], go),
                (w_hbm, w),
                (q_hbm.at[0, 0], qb.at[0]),
            )
        )
    ]
    sign = 1 - 2 * odd
    places = [(FRAME[slot], (0, sign, -sign)[COLUMN[slot]]) for slot in range(9)]
    loads += [
        pltpu.make_async_copy(
            win.at[(t + a + frames) % frames, (h + b + rows_of_tiles) % rows_of_tiles],
            windows.at[slot],
            load_sem.at[5 + slot],
        )
        for slot, (a, b) in enumerate(places)
    ]
    for load in loads:
        load.start()

    def chunk_rows(c):
        return pl.ds(pl.multiple_of(c * ROWS, ROWS), ROWS)

    def tile_copy(name, slot):
        buf, send, recv, source, target, _ = tiles[name]
        return pltpu.make_async_remote_copy(
            src_ref=buf.at[source[slot]],
            dst_ref=buf.at[slot],
            send_sem=send.at[slot],
            recv_sem=recv.at[slot],
            device_id=target[slot],
            device_id_type=MESH,
        )

    def chunk_copy(slot, c):
        rows = chunk_rows(c)
        return pltpu.make_async_remote_copy(
            src_ref=db.at[SOURCE_STRAIGHT[slot], rows],
            dst_ref=db.at[slot, rows],
            send_sem=d_send.at[slot, c],
            recv_sem=d_recv.at[slot, c],
            device_id=straight[slot],
            device_id_type=MESH,
        )

    def rs_copy(kind, c):
        rows = chunk_rows(c)
        return pltpu.make_async_remote_copy(
            src_ref=rs_send.at[kind, rows],
            dst_ref=rs_recv.at[kind, rows],
            send_sem=rs_ssem.at[kind, c],
            recv_sem=rs_rsem.at[kind, c],
            device_id=(x_next, x_prev, x_next, x_next, x_prev, x_prev, y_other)[kind],
            device_id_type=MESH,
        )

    def landed(piece, semaphore):
        pltpu.make_async_copy(piece, piece, semaphore).wait()

    def rs_arrived(kind, c):
        landed(rs_recv.at[kind, chunk_rows(c)], rs_rsem.at[kind, c])

    tiles = {
        "k": (kb, k_send, k_recv, SOURCE, along_z, sends_z),
        "v": (vb, v_send, v_recv, SOURCE, along_z, sends_z),
        "q": (qb, q_send, q_recv, SOURCE, along_z, sends_z),
        "stats": (stats, stats_send, stats_recv, SOURCE_STRAIGHT, straight, sends_z),
    }

    def arrived(name, *slots):
        buf, recv = tiles[name][0], tiles[name][2]
        for slot in slots:
            when(has.get(slot), lambda slot=slot: landed(buf.at[slot], recv.at[slot]))

    def start(name, *slots):
        for slot in slots:
            when(tiles[name][5].get(slot), lambda slot=slot: tile_copy(name, slot).start())

    def chunk_arrived(slot, c):
        when(has.get(slot), lambda: landed(db.at[slot, chunk_rows(c)], d_recv.at[slot, c]))

    def chunk_start(c, *slots):
        for slot in slots:
            when(sends_z.get(slot), lambda slot=slot: chunk_copy(slot, c).start())

    def present(j):
        earlier = (j == 2) | (j == 4) | (j == 7)
        later = (j == 3) | (j == 5) | (j == 8)
        missing = (earlier & (t == 0)) | (later & (t == frames - 1))
        missing = missing | ((j >= 6) & ((h == 0) | (h == rows_of_tiles - 1)))
        return jnp.logical_not(missing)

    def over(first, last, body):
        loop(first, last, lambda j: pl.when(present(j))(lambda: body(j)))

    def partial(column, half, c):
        block = (2 * ((x + column) % RING_X) + (yl if half == 0 else 1 - yl)) * FEAT
        return dot_nt(go[chunk_rows(c), :], w[pl.ds(pl.multiple_of(block, FEAT), FEAT), :])

    def far(c):
        rs_send[0, chunk_rows(c), :] = partial(2, 0, c).astype(bf16)
        rs_send[1, chunk_rows(c), :] = partial(2, 1, c).astype(bf16)

    def near(c):
        rs_send[3, chunk_rows(c), :] = partial(1, 1, c).astype(bf16)
        rs_send[4, chunk_rows(c), :] = partial(3, 0, c).astype(bf16)
        own[0, chunk_rows(c), :] = partial(0, 0, c)
        own[1, chunk_rows(c), :] = partial(0, 1, c)

    loads[2].wait()
    loads[3].wait()
    loop(0, CHUNKS, far)
    loads[0].wait()
    loads[1].wait()

    pl.semaphore_wait(barrier, 4 + sum(jnp.where(condition, 1, 0) for condition, _ in neighbours))

    start("k", 2, 3, 6, 1)

    def far_send(c):
        rs_copy(0, c).start()
        rs_copy(1, c).start()

    loop(0, CHUNKS, far_send)
    start("v", 2, 3, 6, 1)
    loads[4].wait()
    start("q", 6, 1)
    loop(0, CHUNKS, near)

    for slot, (a, b) in enumerate(places):
        loads[5 + slot].wait()
    for slot, (a, b) in enumerate(places):
        seen = windows[0, 0, 9 * (a + 1) + 3 * (b + 1) + 1]
        biases[0, slot] = (seen.astype(f32) - 1.0) * 1e30
        seen = windows[slot, 0, 9 * (1 - a) + 3 * (1 - b) + 1]
        biases[1, slot] = (seen.astype(f32) - 1.0) * 1e30

    heads = [(n, slice(n * HD, (n + 1) * HD)) for n in range(HEADS_HERE)]
    top[...] = jnp.full(top.shape, -1e30, f32)
    for ref in (total, out, dq, dk, dv):
        ref[...] = jnp.zeros(ref.shape, f32)

    def combine(c):
        rs_arrived(0, c)
        rs_send[2, chunk_rows(c), :] = (partial(1, 0, c) + rs_recv[0, chunk_rows(c), :].astype(f32)).astype(bf16)
        rs_copy(2, c).start()
        rs_arrived(1, c)
        rs_send[5, chunk_rows(c), :] = (partial(3, 1, c) + rs_recv[1, chunk_rows(c), :].astype(f32)).astype(bf16)
        rs_copy(5, c).start()
        rs_copy(3, c).start()
        rs_copy(4, c).start()

    loop(0, CHUNKS, combine)

    def scores(j):
        bias = biases[0, j]
        for n, cols in heads:
            s = dot_nt(qb[0, :, cols], kb[j, :, cols]) * (SCALING * LOG2E) + bias
            sbuf[j, n] = s
            highest = top[n]
            for block in BLOCKS:
                highest = jnp.maximum(highest, s[:, block])
            top[n] = highest

    def weights(j):
        for n, cols in heads:
            summed = total[n]
            for block in BLOCKS:
                p = jnp.exp2(sbuf[j, n, :, block] - top[n])
                summed = summed + p
                pq[j, n, :, block] = p.astype(bf16)
            total[n] = summed
            out[n] += dot_nn(pq[j, n], vb[j, :, cols])

    def cross(c):
        rs_arrived(3, c)
        rs_arrived(5, c)
        rs_send[6, chunk_rows(c), :] = (
            own[1, chunk_rows(c), :]
            + rs_recv[3, chunk_rows(c), :].astype(f32)
            + rs_recv[5, chunk_rows(c), :].astype(f32)
        ).astype(bf16)
        rs_copy(6, c).start()

    def settle(c):
        rs_arrived(2, c)
        rs_arrived(4, c)
        summed = (
            own[0, chunk_rows(c), :]
            + rs_recv[2, chunk_rows(c), :].astype(f32)
            + rs_recv[4, chunk_rows(c), :].astype(f32)
        )
        rs_arrived(6, c)
        db[0, chunk_rows(c), :] = (summed + rs_recv[6, chunk_rows(c), :].astype(f32)).astype(bf16)
        chunk_start(c, 2, 3, 6, 1)

    arrived("k", 6, 2, 3)
    start("k", 7, 8, 4, 5)
    arrived("k", 1)
    over(0, 4, scores)
    cross(0)
    arrived("k", 4, 5)
    over(4, 7, scores)
    arrived("v", 6, 2, 3)
    start("v", 7, 8, 4, 5)
    start("q", 2, 3)
    cross(1)
    settle(0)
    arrived("k", 7, 8)
    over(7, 9, scores)
    for n, cols in heads:
        top[n] = spread(jnp.max(top[n], axis=1, keepdims=True))
    cross(2)
    arrived("v", 1, 4, 5)
    over(0, 7, weights)
    settle(1)
    arrived("v", 7, 8)
    over(7, 9, weights)
    for n, cols in heads:
        summed = spread(jnp.sum(total[n], axis=1, keepdims=True))
        top[n] = top[n] + jnp.log(summed) * LOG2E
        total[n] = 1.0 / summed

    def slopes(c):
        rows = chunk_rows(c)
        for n, cols in heads:
            slope = jnp.sum(out[n, rows, :] * db[0, rows, cols].astype(f32), axis=1, keepdims=True)
            mean[n, rows, :] = jnp.broadcast_to(slope, (ROWS, HD)) * total[n, rows, :]

    def query_side(c, j):
        rows = chunk_rows(c)
        for n, cols in heads:
            dp = dot_nt(db[0, rows, cols], vb[j, :, cols])
            slope = mean[n, rows, :]
            ds = jnp.concatenate(
                [(pq[j, n, rows, block].astype(f32) * (dp[:, block] - slope)).astype(bf16) for block in BLOCKS], axis=1
            )
            dq[n, rows, :] += dot_nn(ds, kb[j, :, cols])

    def early(c):
        slopes(c)
        over(0, 9, functools.partial(query_side, c))

    loop(0, CHUNKS - 1, early)
    settle(CHUNKS - 1)
    slopes(CHUNKS - 1)
    columns = [ref[n] for n in range(HEADS_HERE) for ref in (top, mean)]
    lane = lax.broadcasted_iota(jnp.int32, (TILE, HD), 1)
    packed = columns[0]
    for i in range(1, 4):
        packed = jnp.where(lane == i, columns[i], packed)
    stats[0] = packed.T[:8]
    start("stats", 2, 3, 6, 1, 7, 8)
    arrived("q", 6)
    start("q", 7, 8)
    loop(0, CHUNKS, lambda c: chunk_start(c, 7, 8))

    over(0, 9, functools.partial(query_side, CHUNKS - 1))
    arrived("q", 2, 3)
    start("q", 4, 5)

    def key_side(j):
        bias = biases[1, j]
        for n, cols in heads:
            s = dot_nt(kb[0, :, cols], qb[j, :, cols]) * (SCALING * LOG2E) + bias
            p = jnp.exp2(s - stats[j, 2 * n : 2 * n + 1])
            low = p.astype(bf16)
            dv[n] += dot_nn(low, db[j, :, cols])
            dp = dot_nt(vb[0, :, cols], db[j, :, cols])
            ds = (p * (dp - stats[j, 2 * n + 1 : 2 * n + 2])).astype(bf16)
            dk[n] += dot_nn(ds, qb[j, :, cols])

    def sideways(c):
        chunk_arrived(2, c)
        chunk_start(c, 4)
        chunk_arrived(3, c)
        chunk_start(c, 5)

    def ready(*slots):
        arrived("q", *[slot for slot in slots if slot != 6])
        arrived("stats", *slots)
        for slot in slots:
            loop(0, CHUNKS, functools.partial(chunk_arrived, slot))

    ready(1)
    over(0, 2, key_side)
    loop(0, CHUNKS, sideways)
    arrived("stats", 2, 3)
    start("stats", 4, 5)
    for n, cols in heads:
        dq_out[0, 0, :, cols] = (dq[n] * (total[n] * SCALING)).astype(bf16)
    ready(6, 4, 5)
    over(2, 7, key_side)
    ready(7, 8)
    over(7, 9, key_side)
    for n, cols in heads:
        dk_out[0, 0, :, cols] = (dk[n] * SCALING).astype(bf16)
        dv_out[0, 0, :, cols] = dv[n].astype(bf16)

    for slot in range(1, 9):
        for name in tiles:
            when(tiles[name][5].get(slot), lambda name=name, slot=slot: tile_copy(name, slot).wait_send())
        when(
            sends_z.get(slot),
            lambda slot=slot: loop(0, CHUNKS, lambda c: chunk_copy(slot, c).wait_send()),
        )
    for kind in range(7):
        loop(0, CHUNKS, lambda c, kind=kind: rs_copy(kind, c).wait_send())


def deliver(*refs):
    copies = [pltpu.make_async_copy(refs[i], refs[3 + i], refs[6].at[i]) for i in range(3)]
    for copy in copies:
        copy.start()
    for copy in copies:
        copy.wait()


def solution(mesh):
    frames = mesh.shape["tm"]
    rows_of_tiles = mesh.shape["height"]
    dma = pltpu.SemaphoreType.DMA

    def body(grad_output, out_weight, queries, key_states, value_states, window):
        shape = jax.ShapeDtypeStruct((1, 1, TILE, FEAT), bf16)
        hbm = pl.BlockSpec(memory_space=pltpu.HBM)
        vmem = pl.BlockSpec(memory_space=pltpu.VMEM)
        tile = (9, TILE, FEAT)
        column = (HEADS_HERE, TILE, HD)
        results = pl.pallas_call(
            functools.partial(kernel, frames, rows_of_tiles),
            out_shape=(shape, shape, shape),
            in_specs=[hbm] * 6,
            out_specs=[vmem] * 3,
            scratch_shapes=[
                pltpu.VMEM(grad_output.shape[2:], bf16),
                pltpu.VMEM(out_weight.shape, bf16),
                pltpu.VMEM(tile, bf16),
                pltpu.VMEM(tile, bf16),
                pltpu.VMEM(tile, bf16),
                pltpu.VMEM(tile, bf16),
                pltpu.VMEM((9, 8, TILE), f32),
                pltpu.VMEM((9, HEADS_HERE, TILE, TILE), f32),
                pltpu.VMEM((9, HEADS_HERE, TILE, TILE), bf16),
                pltpu.VMEM(column, f32),
                pltpu.VMEM(column, f32),
                pltpu.VMEM(column, f32),
                pltpu.VMEM(column, f32),
                pltpu.VMEM(column, f32),
                pltpu.VMEM(column, f32),
                pltpu.VMEM(column, f32),
                pltpu.VMEM((2, TILE, FEAT), f32),
                pltpu.VMEM((7, TILE, FEAT), bf16),
                pltpu.VMEM((7, TILE, FEAT), bf16),
                pltpu.SMEM((9, 1, 27), jnp.int32),
                pltpu.SMEM((2, 9), f32),
                dma((14,)),
                dma((9,)),
                dma((9,)),
                dma((9,)),
                dma((9,)),
                dma((9,)),
                dma((9,)),
                dma((9, CHUNKS)),
                dma((9, CHUNKS)),
                dma((9,)),
                dma((9,)),
                dma((7, CHUNKS)),
                dma((7, CHUNKS)),
            ],
            compiler_params=pltpu.CompilerParams(
                collective_id=0, has_side_effects=True, vmem_limit_bytes=54400 * 1024
            ),
        )(grad_output, out_weight, queries, key_states, value_states, window)
        return pl.pallas_call(
            deliver,
            out_shape=(shape, shape, shape),
            in_specs=[vmem] * 3,
            out_specs=[hbm] * 3,
            scratch_shapes=[dma((3,))],
            compiler_params=pltpu.CompilerParams(vmem_limit_bytes=4096 * 1024),
        )(*results)

    split = P("tm", "height", None, "heads")
    return jax.shard_map(
        body,
        mesh=mesh,
        in_specs=(split, P(None, "heads"), split, split, split, P()),
        out_specs=(split, split, split),
        check_vma=False,
    )
```

```python
import functools

import jax
import jax.numpy as jnp
from jax import lax
from jax.experimental import pallas as pl
from jax.experimental.pallas import tpu as pltpu
from jax.sharding import PartitionSpec as P

HD = 128
TILE = 384
FEAT = 256
HEADS_HERE = 2
CHUNKS = 3
ROWS = TILE // CHUNKS
RING_X = 4
LOG2E = 1.4426950408889634
SCALING = HD ** (-0.5)
MESH = pl.DeviceIdType.MESH

FRAME = (0, 0, -1, 1, -1, 1, 0, -1, 1)
COLUMN = (0, 1, 0, 0, 1, 1, 2, 2, 2)
SOURCE = {1: 0, 2: 0, 3: 0, 6: 0, 4: 2, 5: 3, 7: 6, 8: 6}
SOURCE_STRAIGHT = {**SOURCE, 7: 0, 8: 0}
BLOCKS = tuple(slice(i * HD, (i + 1) * HD) for i in range(TILE // HD))

f32 = jnp.float32
bf16 = jnp.bfloat16


def dot_nt(a, b):
    return lax.dot_general(a, b, (((1,), (1,)), ((), ())), preferred_element_type=f32)


def dot_tn(a, b):
    return lax.dot_general(a, b, (((0,), (0,)), ((), ())), preferred_element_type=f32)


def dot_nn(a, b):
    return lax.dot_general(a, b, (((1,), (0,)), ((), ())), preferred_element_type=f32)


def loop(first, last, body):
    def step(index, carry):
        body(index)
        return carry

    lax.fori_loop(first, last, step, 0)


def when(condition, action):
    if condition is None:
        action()
    else:
        pl.when(condition)(action)


def spread(column):
    return jnp.broadcast_to(column, (TILE, HD))


def kernel(
    frames,
    rows_of_tiles,
    go_hbm,
    w_hbm,
    q_hbm,
    k_hbm,
    v_hbm,
    win,
    dq_out,
    dk_out,
    dv_out,
    go,
    w,
    kb,
    vb,
    qb,
    db,
    stats,
    sbuf,
    pq,
    top,
    total,
    mean,
    out,
    dq,
    dk,
    dv,
    own,
    rs_send,
    rs_recv,
    windows,
    biases,
    load_sem,
    k_send,
    k_recv,
    v_send,
    v_recv,
    q_send,
    q_recv,
    d_send,
    d_recv,
    stats_send,
    stats_recv,
    rs_ssem,
    rs_rsem,
):
    t = lax.axis_index("tm")
    h = lax.axis_index("height")
    g = lax.axis_index("heads")
    x = g // 2
    yl = g % 2
    odd = h % 2
    before = t > 0
    after = t < frames - 1
    beside = (h > 0) & (h < rows_of_tiles - 1)
    partner = {"height": h + 1 - 2 * odd}
    outer = {"height": (h + 2 * odd - 1 + rows_of_tiles) % rows_of_tiles}
    t_next = {"tm": (t + 1) % frames}
    t_prev = {"tm": (t + frames - 1) % frames}
    x_next = {"heads": ((x + 1) % RING_X) * 2 + yl}
    x_prev = {"heads": ((x + RING_X - 1) % RING_X) * 2 + yl}
    y_other = {"heads": x * 2 + 1 - yl}
    has = {2: before, 3: after, 4: before, 5: after, 6: beside, 7: before & beside, 8: after & beside}
    along_z = {1: partner, 4: partner, 5: partner, 2: t_next, 7: t_next, 3: t_prev, 8: t_prev, 6: outer}
    sends_z = {4: before, 5: after, 2: after, 7: after & beside, 3: before, 8: before & beside, 6: beside}
    straight = {**along_z, 7: {**t_next, **outer}, 8: {**t_prev, **outer}}

    barrier = pltpu.get_barrier_semaphore()

    def greet(peer):
        pl.semaphore_signal(barrier, inc=1, device_id=peer, device_id_type=MESH)

    for peer in (partner, x_next, x_prev, y_other):
        greet(peer)
    neighbours = ((before, t_prev), (after, t_next), (beside, outer), (sends_z[7], straight[7]), (sends_z[8], straight[8]))
    for condition, peer in neighbours:
        when(condition, functools.partial(greet, peer))

    loads = [
        pltpu.make_async_copy(src, dst, load_sem.at[i])
        for i, (src, dst) in enumerate(
            (
                (k_hbm.at[0, 0], kb.at[0]),
                (v_hbm.at[0, 0], vb.at[0]),
                (go_hbm.at[0, 0], go),
                (w_hbm, w),
                (q_hbm.at[0, 0], qb.at[0]),
            )
        )
    ]
    sign = 1 - 2 * odd
    places = [(FRAME[slot], (0, sign, -sign)[COLUMN[slot]]) for slot in range(9)]
    loads += [
        pltpu.make_async_copy(
            win.at[(t + a + frames) % frames, (h + b + rows_of_tiles) % rows_of_tiles],
            windows.at[slot],
            load_sem.at[5 + slot],
        )
        for slot, (a, b) in enumerate(places)
    ]
    for load in loads:
        load.start()

    def chunk_rows(c):
        return pl.ds(pl.multiple_of(c * ROWS, ROWS), ROWS)

    def tile_copy(name, slot):
        buf, send, recv, source, target, _ = tiles[name]
        return pltpu.make_async_remote_copy(
            src_ref=buf.at[source[slot]],
            dst_ref=buf.at[slot],
            send_sem=send.at[slot],
            recv_sem=recv.at[slot],
            device_id=target[slot],
            device_id_type=MESH,
        )

    def chunk_copy(slot, c):
        rows = chunk_rows(c)
        return pltpu.make_async_remote_copy(
            src_ref=db.at[SOURCE_STRAIGHT[slot], rows],
            dst_ref=db.at[slot, rows],
            send_sem=d_send.at[slot, c],
            recv_sem=d_recv.at[slot, c],
            device_id=straight[slot],
            device_id_type=MESH,
        )

    def rs_copy(kind, c):
        rows = chunk_rows(c)
        return pltpu.make_async_remote_copy(
            src_ref=rs_send.at[kind, rows],
            dst_ref=rs_recv.at[kind, rows],
            send_sem=rs_ssem.at[kind, c],
            recv_sem=rs_rsem.at[kind, c],
            device_id=(x_next, x_prev, x_next, x_next, x_prev, x_prev, y_other)[kind],
            device_id_type=MESH,
        )

    def landed(piece, semaphore):
        pltpu.make_async_copy(piece, piece, semaphore).wait()

    def rs_arrived(kind, c):
        landed(rs_recv.at[kind, chunk_rows(c)], rs_rsem.at[kind, c])

    tiles = {
        "k": (kb, k_send, k_recv, SOURCE, along_z, sends_z),
        "v": (vb, v_send, v_recv, SOURCE, along_z, sends_z),
        "q": (qb, q_send, q_recv, SOURCE, along_z, sends_z),
        "stats": (stats, stats_send, stats_recv, SOURCE_STRAIGHT, straight, sends_z),
    }

    def arrived(name, *slots):
        buf, recv = tiles[name][0], tiles[name][2]
        for slot in slots:
            when(has.get(slot), lambda slot=slot: landed(buf.at[slot], recv.at[slot]))

    def start(name, *slots):
        for slot in slots:
            when(tiles[name][5].get(slot), lambda slot=slot: tile_copy(name, slot).start())

    def chunk_arrived(slot, c):
        when(has.get(slot), lambda: landed(db.at[slot, chunk_rows(c)], d_recv.at[slot, c]))

    def chunk_start(c, *slots):
        for slot in slots:
            when(sends_z.get(slot), lambda slot=slot: chunk_copy(slot, c).start())

    def present(j):
        earlier = (j == 2) | (j == 4) | (j == 7)
        later = (j == 3) | (j == 5) | (j == 8)
        missing = (earlier & (t == 0)) | (later & (t == frames - 1))
        missing = missing | ((j >= 6) & ((h == 0) | (h == rows_of_tiles - 1)))
        return jnp.logical_not(missing)

    def over(first, last, body):
        loop(first, last, lambda j: pl.when(present(j))(lambda: body(j)))

    def partial(column, half, c):
        block = (2 * ((x + column) % RING_X) + (yl if half == 0 else 1 - yl)) * FEAT
        return dot_nt(go[chunk_rows(c), :], w[pl.ds(pl.multiple_of(block, FEAT), FEAT), :])

    def far(c):
        rs_send[0, chunk_rows(c), :] = partial(2, 0, c).astype(bf16)
        rs_send[1, chunk_rows(c), :] = partial(2, 1, c).astype(bf16)

    def near(c):
        rs_send[3, chunk_rows(c), :] = partial(1, 1, c).astype(bf16)
        rs_send[4, chunk_rows(c), :] = partial(3, 0, c).astype(bf16)
        own[0, chunk_rows(c), :] = partial(0, 0, c)
        own[1, chunk_rows(c), :] = partial(0, 1, c)

    loads[2].wait()
    loads[3].wait()
    loop(0, CHUNKS, far)
    loads[0].wait()
    loads[1].wait()

    pl.semaphore_wait(barrier, 4 + sum(jnp.where(condition, 1, 0) for condition, _ in neighbours))

    start("k", 2, 3, 6, 1)

    def far_send(c):
        rs_copy(0, c).start()
        rs_copy(1, c).start()

    loop(0, CHUNKS, far_send)
    start("v", 2, 3, 6, 1)
    loads[4].wait()
    start("q", 6, 1)
    loop(0, CHUNKS, near)

    for slot, (a, b) in enumerate(places):
        loads[5 + slot].wait()
    for slot, (a, b) in enumerate(places):
        seen = windows[0, 0, 9 * (a + 1) + 3 * (b + 1) + 1]
        biases[0, slot] = (seen.astype(f32) - 1.0) * 1e30
        seen = windows[slot, 0, 9 * (1 - a) + 3 * (1 - b) + 1]
        biases[1, slot] = (seen.astype(f32) - 1.0) * 1e30

    heads = [(n, slice(n * HD, (n + 1) * HD)) for n in range(HEADS_HERE)]
    top[...] = jnp.full(top.shape, -1e30, f32)
    for ref in (total, out, dq, dk, dv):
        ref[...] = jnp.zeros(ref.shape, f32)

    def combine(c):
        rs_arrived(0, c)
        rs_send[2, chunk_rows(c), :] = (partial(1, 0, c) + rs_recv[0, chunk_rows(c), :].astype(f32)).astype(bf16)
        rs_copy(2, c).start()
        rs_arrived(1, c)
        rs_send[5, chunk_rows(c), :] = (partial(3, 1, c) + rs_recv[1, chunk_rows(c), :].astype(f32)).astype(bf16)
        rs_copy(5, c).start()
        rs_copy(3, c).start()
        rs_copy(4, c).start()

    loop(0, CHUNKS, combine)

    def scores(j):
        bias = biases[0, j]
        for n, cols in heads:
            s = dot_nt(qb[0, :, cols], kb[j, :, cols]) * (SCALING * LOG2E) + bias
            sbuf[j, n] = s
            highest = top[n]
            for block in BLOCKS:
                highest = jnp.maximum(highest, s[:, block])
            top[n] = highest

    def weights(j):
        for n, cols in heads:
            summed = total[n]
            for block in BLOCKS:
                p = jnp.exp2(sbuf[j, n, :, block] - top[n])
                summed = summed + p
                pq[j, n, :, block] = p.astype(bf16)
            total[n] = summed
            out[n] += dot_nn(pq[j, n], vb[j, :, cols])

    def cross(c):
        rs_arrived(3, c)
        rs_arrived(5, c)
        rs_send[6, chunk_rows(c), :] = (
            own[1, chunk_rows(c), :]
            + rs_recv[3, chunk_rows(c), :].astype(f32)
            + rs_recv[5, chunk_rows(c), :].astype(f32)
        ).astype(bf16)
        rs_copy(6, c).start()

    def settle(c):
        rs_arrived(2, c)
        rs_arrived(4, c)
        summed = (
            own[0, chunk_rows(c), :]
            + rs_recv[2, chunk_rows(c), :].astype(f32)
            + rs_recv[4, chunk_rows(c), :].astype(f32)
        )
        rs_arrived(6, c)
        db[0, chunk_rows(c), :] = (summed + rs_recv[6, chunk_rows(c), :].astype(f32)).astype(bf16)
        chunk_start(c, 2, 3, 6, 1)

    arrived("k", 6, 2, 3)
    start("k", 7, 8, 4, 5)
    arrived("k", 1)
    over(0, 4, scores)
    cross(0)
    arrived("k", 4, 5)
    over(4, 7, scores)
    arrived("v", 6, 2, 3)
    start("v", 7, 8, 4, 5)
    start("q", 2, 3)
    cross(1)
    settle(0)
    cross(2)
    settle(1)
    settle(2)
    arrived("q", 6)
    start("q", 7, 8)
    arrived("k", 7, 8)
    over(7, 9, scores)
    for n, cols in heads:
        top[n] = spread(jnp.max(top[n], axis=1, keepdims=True))
    arrived("v", 1, 4, 5)
    over(0, 7, weights)
    arrived("v", 7, 8)
    over(7, 9, weights)

    columns = []
    for n, cols in heads:
        summed = spread(jnp.sum(total[n], axis=1, keepdims=True))
        inverse = 1.0 / summed
        total[n] = inverse
        columns.append(top[n] + jnp.log(summed) * LOG2E)
        slope = jnp.sum(out[n] * db[0, :, cols].astype(f32), axis=1, keepdims=True)
        mean[n] = spread(slope) * inverse
        columns.append(mean[n])
    lane = lax.broadcasted_iota(jnp.int32, (TILE, HD), 1)
    packed = columns[0]
    for i in range(1, 4):
        packed = jnp.where(lane == i, columns[i], packed)
    stats[0] = packed.T[:8]
    start("stats", 2, 3, 6, 1, 7, 8)
    loop(0, CHUNKS, lambda c: chunk_start(c, 7, 8))

    def query_side(j):
        for n, cols in heads:
            dp = dot_nt(db[0, :, cols], vb[j, :, cols])
            ds = jnp.concatenate(
                [(pq[j, n, :, block].astype(f32) * (dp[:, block] - mean[n])).astype(bf16) for block in BLOCKS], axis=1
            )
            dq[n] += dot_nn(ds, kb[j, :, cols])

    over(0, 7, query_side)
    arrived("q", 2, 3)
    start("q", 4, 5)
    over(7, 9, query_side)

    def key_side(j):
        bias = biases[1, j]
        for n, cols in heads:
            s = dot_nt(kb[0, :, cols], qb[j, :, cols]) * (SCALING * LOG2E) + bias
            p = jnp.exp2(s - stats[j, 2 * n : 2 * n + 1])
            low = p.astype(bf16)
            dv[n] += dot_nn(low, db[j, :, cols])
            dp = dot_nt(vb[0, :, cols], db[j, :, cols])
            ds = (p * (dp - stats[j, 2 * n + 1 : 2 * n + 2])).astype(bf16)
            dk[n] += dot_nn(ds, qb[j, :, cols])

    def sideways(c):
        chunk_arrived(2, c)
        chunk_start(c, 4)
        chunk_arrived(3, c)
        chunk_start(c, 5)

    def ready(*slots):
        arrived("q", *[slot for slot in slots if slot != 6])
        arrived("stats", *slots)
        for slot in slots:
            loop(0, CHUNKS, functools.partial(chunk_arrived, slot))

    ready(1)
    over(0, 2, key_side)
    loop(0, CHUNKS, sideways)
    arrived("stats", 2, 3)
    start("stats", 4, 5)
    for n, cols in heads:
        dq_out[0, 0, :, cols] = (dq[n] * (total[n] * SCALING)).astype(bf16)
    ready(6, 4, 5)
    over(2, 7, key_side)
    ready(7, 8)
    over(7, 9, key_side)
    for n, cols in heads:
        dk_out[0, 0, :, cols] = (dk[n] * SCALING).astype(bf16)
        dv_out[0, 0, :, cols] = dv[n].astype(bf16)

    for slot in range(1, 9):
        for name in tiles:
            when(tiles[name][5].get(slot), lambda name=name, slot=slot: tile_copy(name, slot).wait_send())
        when(
            sends_z.get(slot),
            lambda slot=slot: loop(0, CHUNKS, lambda c: chunk_copy(slot, c).wait_send()),
        )
    for kind in range(7):
        loop(0, CHUNKS, lambda c, kind=kind: rs_copy(kind, c).wait_send())


def deliver(*refs):
    copies = [pltpu.make_async_copy(refs[i], refs[3 + i], refs[6].at[i]) for i in range(3)]
    for copy in copies:
        copy.start()
    for copy in copies:
        copy.wait()


def solution(mesh):
    frames = mesh.shape["tm"]
    rows_of_tiles = mesh.shape["height"]
    dma = pltpu.SemaphoreType.DMA

    def body(grad_output, out_weight, queries, key_states, value_states, window):
        shape = jax.ShapeDtypeStruct((1, 1, TILE, FEAT), bf16)
        hbm = pl.BlockSpec(memory_space=pltpu.HBM)
        vmem = pl.BlockSpec(memory_space=pltpu.VMEM)
        tile = (9, TILE, FEAT)
        column = (HEADS_HERE, TILE, HD)
        results = pl.pallas_call(
            functools.partial(kernel, frames, rows_of_tiles),
            out_shape=(shape, shape, shape),
            in_specs=[hbm] * 6,
            out_specs=[vmem] * 3,
            scratch_shapes=[
                pltpu.VMEM(grad_output.shape[2:], bf16),
                pltpu.VMEM(out_weight.shape, bf16),
                pltpu.VMEM(tile, bf16),
                pltpu.VMEM(tile, bf16),
                pltpu.VMEM(tile, bf16),
                pltpu.VMEM(tile, bf16),
                pltpu.VMEM((9, 8, TILE), f32),
                pltpu.VMEM((9, HEADS_HERE, TILE, TILE), f32),
                pltpu.VMEM((9, HEADS_HERE, TILE, TILE), bf16),
                pltpu.VMEM(column, f32),
                pltpu.VMEM(column, f32),
                pltpu.VMEM(column, f32),
                pltpu.VMEM(column, f32),
                pltpu.VMEM(column, f32),
                pltpu.VMEM(column, f32),
                pltpu.VMEM(column, f32),
                pltpu.VMEM((2, TILE, FEAT), f32),
                pltpu.VMEM((7, TILE, FEAT), bf16),
                pltpu.VMEM((7, TILE, FEAT), bf16),
                pltpu.SMEM((9, 1, 27), jnp.int32),
                pltpu.SMEM((2, 9), f32),
                dma((14,)),
                dma((9,)),
                dma((9,)),
                dma((9,)),
                dma((9,)),
                dma((9,)),
                dma((9,)),
                dma((9, CHUNKS)),
                dma((9, CHUNKS)),
                dma((9,)),
                dma((9,)),
                dma((7, CHUNKS)),
                dma((7, CHUNKS)),
            ],
            compiler_params=pltpu.CompilerParams(
                collective_id=0, has_side_effects=True, vmem_limit_bytes=54400 * 1024
            ),
        )(grad_output, out_weight, queries, key_states, value_states, window)
        return pl.pallas_call(
            deliver,
            out_shape=(shape, shape, shape),
            in_specs=[vmem] * 3,
            out_specs=[hbm] * 3,
            scratch_shapes=[dma((3,))],
            compiler_params=pltpu.CompilerParams(vmem_limit_bytes=4096 * 1024),
        )(*results)

    split = P("tm", "height", None, "heads")
    return jax.shard_map(
        body,
        mesh=mesh,
        in_specs=(split, P(None, "heads"), split, split, split, P()),
        out_specs=(split, split, split),
        check_vma=False,
    )
```
